32 devices in a mesh: row: 8 (over z, core), col: 4 (over y, x).
Axes of the slice: x: 2, y: 2, z: 4, core: 2. Of those that a mesh axis runs over, the one named last changes fastest.
Arguments:
- vectors: bfloat16 [2, 4, 16384], P(None, 'col', 'row'), may hold values from -6 to 6
- lr_left: bfloat16 [8, 4, 32, 8, 2048], P('row', 'col'), may hold values from -0.75 to 0.75
- lr_right: bfloat16 [8, 4, 32, 8, 2048], P('row', 'col'), may hold values from -0.125 to 0.125
- tile_rank: int32 [8, 4, 32], P('row', 'col'), may hold values from 0 to 8, as said below
- leaf_values: bfloat16 [8, 4, 8, 512, 512], P('row', 'col'), may hold values from -0.25 to 0.25
- leaf_places: int32 [8, 4, 8, 2], P('row', 'col'), may hold values from 0 to 31, as said below
- cluster_perm: int32 [8, 8192], P('row'), may hold values from 0 to 65535, as said below
- kappa: float32 [32, 16, 128], P('row', 'col'), may hold values from 0.25 to 4
Outputs:
- prior_action: float32 [2, 32, 16, 128], P(None, 'row', 'col')
The draws below stay inside these ranges and needn't reach their ends.
Inputs may be any that keep to these rules, and one draw needn't show every extreme that they name: `tile_rank`: 0 exactly on the tiles that contain a leaf, 1 to 8 on the others. `leaf_places`: the 8 leaves of a block are distinct; entry 0 indexes rows and entry 1 column of the block in units of 512. `cluster_perm`: a permutation of all brick indices; within each aligned block of 2048 entries, every value of entry // 2048 occurs exactly 128 times or not at all.
All inputs are finite; a program needn't handle non-finite values.
Results may differ from the reference program's by a relative error of at most 0.0023.
Values may be sent and summed in bfloat16 or wider, within the bound.
A program may use at most 64 MiB of HBM per device.

```python
import math
import jax
import jax.numpy as jnp
from jax import lax

NVEC = 2
CX = 4
CY = 4
NZ = 128
TILE_ROWS = 4
TILE_COLS = 8
KMAX = 8
LEAF = 512
NLEAF = 8
PTS_DEV = 2048
BLOCK_ROWS = 8
BLOCK_COLS = 4
ROWS_CL = 8192
COLS_CL = 16384
TS = 2048
NX = 32
NY = 16
POINTS = 65536
CAP = 128
DEVICES = 32


def leaf_layout(key):
    base = jax.random.fold_in(key, 11)
    row_count = ROWS_CL // LEAF
    col_count = COLS_CL // LEAF
    every_key = jax.random.split(base, BLOCK_ROWS * BLOCK_COLS)

    def one_block(single):
        chosen = jax.random.permutation(single, row_count * col_count)[:NLEAF]
        return jnp.stack([chosen // col_count, chosen % col_count], axis=1)
    places = jax.vmap(one_block)(every_key)
    return places.reshape(BLOCK_ROWS, BLOCK_COLS, NLEAF, 2).astype(jnp.int32)


def draw_leaf_places(key, part):
    return leaf_layout(key)


def draw_tile_rank(key, part):
    places = leaf_layout(key)
    tile_ranks = jax.random.randint(jax.random.fold_in(key, 12), (BLOCK_ROWS, BLOCK_COLS, TILE_ROWS * TILE_COLS), 1, KMAX + 1)
    tile_of = places[..., 0] * LEAF // TS * TILE_COLS + places[..., 1] * LEAF // TS
    near_tile = jnp.any(tile_of[..., :, None] == jnp.arange(TILE_ROWS * TILE_COLS)[None, None, None, :], axis=2)
    return jnp.where(near_tile, 0, tile_ranks).astype(jnp.int32)


def draw_cluster_perm(key, part):
    base = jax.random.fold_in(key, 21)
    keys_a, keys_b, keys_c = jax.random.split(base, 3)
    group_total = PTS_DEV // CAP
    offsets = jax.random.permutation(keys_a, DEVICES)[:group_total]
    shuffle = jax.vmap(lambda single: jax.random.permutation(single, PTS_DEV))(jax.random.split(keys_b, DEVICES))
    landing = jax.vmap(lambda single: jax.random.permutation(single, PTS_DEV))(jax.random.split(keys_c, DEVICES))
    source = jnp.arange(DEVICES)[:, None]
    group_id = shuffle // CAP
    target = (source + offsets[group_id]) % DEVICES
    landing_spot = landing[target, shuffle]
    return (target * PTS_DEV + landing_spot).reshape(BLOCK_ROWS, ROWS_CL).astype(jnp.int32)


def levels(own_key, shape, shards, least, largest):
    gain, own = 1.0, jax.random.fold_in(own_key, 6)
    for axis_at, blocks in shards:
        heights = jnp.exp(jax.random.uniform(jax.random.fold_in(own, axis_at), (blocks,), jnp.float32, least / len(shards), largest / len(shards)))
        gain = gain * jnp.repeat(heights, shape[axis_at] // blocks).reshape([-1 if axis == axis_at else 1 for axis in range(len(shape))])
    return gain


def noise(rng, dims, scale, limit, shards=(), held_as=jnp.bfloat16):
    drawn = scale * jax.random.normal(rng, dims, jnp.float32)
    if shards:
        drawn = drawn * levels(rng, dims, shards, -0.22, 0.18)
    return jnp.clip(drawn, -limit, limit).astype(held_as)


def setup_inputs(seed: int = 0) -> dict:
    key_list = jax.random.split(jax.random.key(seed), 9)
    return {
        "vectors": noise(key_list[0], (NVEC, BLOCK_COLS, COLS_CL), 1.0, 6.0, ((1, 4), (2, 8))),
        "lr_left": noise(key_list[1], (BLOCK_ROWS, BLOCK_COLS, TILE_ROWS * TILE_COLS, KMAX, TS), (KMAX * TILE_COLS) ** -0.5, 0.75, ((0, 8), (1, 4))),
        "lr_right": noise(key_list[2], (BLOCK_ROWS, BLOCK_COLS, TILE_ROWS * TILE_COLS, KMAX, TS), TS ** -0.5, 0.125, ((0, 8), (1, 4))),
        "tile_rank": draw_tile_rank(jax.random.fold_in(key_list[8], 71), 0),
        "leaf_values": noise(key_list[4], (BLOCK_ROWS, BLOCK_COLS, NLEAF, LEAF, LEAF), LEAF ** -0.5, 0.25, ((0, 8), (1, 4))),
        "leaf_places": draw_leaf_places(jax.random.fold_in(key_list[8], 71), 0),
        "cluster_perm": draw_cluster_perm(jax.random.fold_in(key_list[8], 71), 0),
        "kappa": jnp.clip(jnp.exp(math.log(4.0) - 2.7725887 * jax.random.uniform(key_list[7], (NX, NY, NZ), jnp.float32) ** levels(key_list[7], (NX, NY, NZ), ((0, 8), (1, 4)), -0.2, 0.2)), 0.25, 4.0),
    }


def prior_step(padded, stiffness):
    center = padded[:, 1:-1, 1:-1, :]
    flat_pad = jnp.pad(center, ((0, 0), (0, 0), (0, 0), (1, 1)))
    beside = padded[:, 2:, 1:-1, :] + padded[:, :-2, 1:-1, :]
    beside = beside + padded[:, 1:-1, 2:, :] + padded[:, 1:-1, :-2, :]
    beside = beside + flat_pad[..., 2:] + flat_pad[..., :-2]
    return ((6.0 + stiffness) * center - beside) * 0.125


def block_product(far_left, far_right, tile_ranks, leaf_vals, leaf_pos, x_column):
    x_tiles = x_column.reshape(NVEC, TILE_COLS, TS).astype(jnp.float32)
    right_tiles = far_right.reshape(TILE_ROWS, TILE_COLS, KMAX, TS).astype(jnp.float32)
    projected = jnp.einsum('abkp,vbp->abvk', right_tiles, x_tiles)
    rank_mask = (jnp.arange(KMAX)[None, None, :] < tile_ranks.reshape(TILE_ROWS, TILE_COLS)[:, :, None]).astype(jnp.float32)
    projected = lax.optimization_barrier((projected * rank_mask[:, :, None, :]).astype(jnp.bfloat16)).astype(jnp.float32)
    left_tiles = far_left.reshape(TILE_ROWS, TILE_COLS, KMAX, TS).astype(jnp.float32)
    far_part = jnp.einsum('abkp,abvk->vap', left_tiles, projected).reshape(NVEC, ROWS_CL)
    x_sub = x_column.reshape(NVEC, COLS_CL // LEAF, LEAF).astype(jnp.float32)
    picked = x_sub[:, leaf_pos[:, 1], :]
    near_out = jnp.einsum('lqp,vlp->vlq', leaf_vals.astype(jnp.float32), picked)
    near_part = jnp.zeros((NVEC, ROWS_CL // LEAF, LEAF), jnp.float32).at[:, leaf_pos[:, 0], :].add(near_out)
    return far_part + near_part.reshape(NVEC, ROWS_CL)


def reference(vectors, lr_left, lr_right, tile_rank, leaf_values, leaf_places, cluster_perm, kappa):
    columns = jnp.transpose(vectors, (1, 0, 2))

    def one_row(inputs):
        left_row, right_row, rank_row, vals_row, pos_row = inputs

        def add_block(carry, column):
            left_one, right_one, rank_one, vals_one, pos_one, x_one = column
            return carry + block_product(left_one, right_one, rank_one, vals_one, pos_one, x_one), None

        summed, unused = lax.scan(add_block, jnp.zeros((NVEC, ROWS_CL), jnp.float32),
                                  (left_row, right_row, rank_row, vals_row, pos_row, columns))
        return summed

    sums = lax.map(one_row, (lr_left, lr_right, tile_rank, leaf_values, leaf_places))
    action = jnp.transpose(sums, (1, 0, 2)).reshape(NVEC, POINTS)
    bricks = jnp.zeros((NVEC, POINTS), jnp.float32).at[:, cluster_perm.reshape(-1)].set(action)
    field = bricks.reshape(NVEC, BLOCK_ROWS, BLOCK_COLS, CX, CY, NZ)
    field = jnp.transpose(field, (0, 1, 3, 2, 4, 5)).reshape(NVEC, NX, NY, NZ)
    for repeat in range(4):
        padded = jnp.pad(field, ((0, 0), (1, 1), (1, 1), (0, 0)))
        field = prior_step(padded, kappa)
    return field
```

```python
import functools

import jax
import jax.numpy as jnp
from jax import lax
from jax.experimental import pallas as pl
from jax.experimental.pallas import tpu as pltpu
from jax.sharding import PartitionSpec as P

CX = 4
CY = 4
TILE_ROWS = 4
TILE_COLS = 8
LANES = 128
MESH = pl.DeviceIdType.MESH
F32 = jnp.float32
BF16 = jnp.bfloat16
NT = (((1,), (1,)), ((), ()))
SIDES = [(-1, -1), (-1, 1), (1, -1), (1, 1), (0, -1), (0, 1), (-1, 0), (1, 0)]


def dot_nt(a, b):
    return lax.dot_general(a, b, NT, preferred_element_type=F32)


def pieces(x):
    first = x.astype(BF16)
    return first, (x - first.astype(F32)).astype(BF16)


def iota(shape, dim):
    return lax.broadcasted_iota(jnp.int32, shape, dim)


def kernel(
    rows, cols, kmax, leaf,
    x_hbm, right_hbm, left_hbm, rank_hbm, leaf_hbm, places_hbm, perm_hbm, kappa_hbm,
    out_ref,
    rank_ref, places_ref, corner, hc, perm_ref, kappa_ref, right_ref, left_ref, leaf_ref, xg, x32, slot_hot, dest_hot,
    msend, rm, vsend, rv, lane_hot, hit_hot, brick, hb, kb, ext, coef, scale,
    local_sem, ag_sem, m_sem, v_send, v_recv, k_send, k_recv, h_send, h_recv,
):
    subs, nvec = x_hbm.shape[:2]
    points = subs * leaf
    tile = right_ref.shape[1]
    taps = right_ref.shape[0]
    devices = rows * cols
    nleaf = leaf_ref.shape[0]
    cells = CX * CY
    blocks = points // LANES
    r = lax.axis_index("row")
    c = lax.axis_index("col")
    me = r * cols + c

    own_x = pltpu.make_async_copy(x_hbm, xg.at[r], local_sem.at[3])
    own_perm = pltpu.make_async_copy(perm_hbm, perm_ref, local_sem.at[4])
    own_kappa = pltpu.make_async_copy(kappa_hbm, kappa_ref, local_sem.at[5])
    small = [
        pltpu.make_async_copy(rank_hbm, rank_ref, local_sem.at[6]),
        pltpu.make_async_copy(places_hbm, places_ref, local_sem.at[7]),
    ]
    loads = [
        pltpu.make_async_copy(right_hbm, right_ref, local_sem.at[0]),
        pltpu.make_async_copy(left_hbm, left_ref, local_sem.at[1]),
        pltpu.make_async_copy(leaf_hbm, leaf_ref, local_sem.at[2]),
    ]

    def turned(place, by, count):
        moved = place + by
        return moved - jnp.where(moved >= count, count, 0)

    def mirrored(place, by, count):
        if count & (count - 1):
            return turned(place, by, count)
        moved, bit = place, 1
        while bit <= by:
            if by & bit:
                moved = moved + bit - 2 * bit * (place // bit % 2)
            bit *= 2
        return moved

    def far(by):
        return bin(by).count("1")

    row_order = sorted(range(1, rows), key=lambda k: -k)
    col_order = sorted(range(1, cols), key=lambda k: -far(k))
    all_order = sorted(
        ((dr, dc) for dr in range(rows) for dc in range(cols) if dr + dc),
        key=lambda d: -(d[0] // 2 + far(d[1]) + 0.5 * (d[0] % 2)),
    )

    barrier = pltpu.get_barrier_semaphore()
    for k in row_order:
        pl.semaphore_signal(
            barrier, inc=1, device_id={"row": mirrored(r, k, rows), "col": c}, device_id_type=MESH
        )
    for k in col_order:
        pl.semaphore_signal(
            barrier, inc=1, device_id={"row": r, "col": mirrored(c, k, cols)}, device_id_type=MESH
        )
    for load in [own_x, own_perm] + small + [own_kappa] + loads:
        load.start()
    own_x.wait()
    pl.semaphore_wait(barrier, rows + cols - 2)
    for k in row_order:
        pltpu.make_async_remote_copy(
            src_ref=xg.at[r], dst_ref=xg.at[r], send_sem=ag_sem.at[0], recv_sem=ag_sem.at[1],
            device_id={"row": mirrored(r, k, rows), "col": c}, device_id_type=MESH,
        ).start()

    own_perm.wait()
    dev_ids = iota((devices, LANES), 0)
    lane_rows = iota((LANES, LANES), 0).astype(F32)
    ahead = (iota((LANES, 2 * LANES), 0) < iota((LANES, 2 * LANES), 1)).astype(BF16)
    for j in range(cols):
        dev_of = perm_ref[j * blocks : (j + 1) * blocks, :] // points
        hots = [(dev_of[b : b + 1, :] == dev_ids).astype(F32) for b in range(blocks)]
        all_hot = jnp.concatenate(hots, axis=0).astype(BF16)
        counts = jnp.dot(all_hot, ahead, preferred_element_type=F32)
        offset = jnp.zeros((devices, LANES), F32)
        for b in range(blocks):
            span = slice(b * devices, (b + 1) * devices)
            at = (j * blocks + b) * LANES
            rank = jnp.sum(hots[b] * (counts[span, :LANES] + offset), axis=0, keepdims=True)
            offset = offset + counts[span, LANES:]
            slot_hot[:, at : at + LANES] = (rank == lane_rows).astype(BF16)
            dest_hot[:, at : at + LANES] = all_hot[span]
    mine = pl.ds(pl.multiple_of(c * points, LANES), points)
    place = perm_ref[pl.ds(pl.multiple_of(c * blocks, 8), blocks), :] % points
    halves = ((place // LANES).astype(F32), (place % LANES).astype(F32))
    dest_mine = dest_hot[:, mine]
    meta = jnp.concatenate(
        [
            jnp.concatenate(
                [
                    dest_mine[:, b * LANES : (b + 1) * LANES]
                    * jnp.broadcast_to(half[b : b + 1, :], (devices, LANES)).astype(BF16)
                    for b in range(blocks)
                ],
                axis=1,
            )
            for half in halves
        ],
        axis=0,
    )
    meta = dot_nt(meta, slot_hot[:, mine])
    for h in range(2):
        msend[:, h, :] = meta[h * devices : (h + 1) * devices]
    for load in small:
        load.wait()
    wide = TILE_COLS * nvec
    lane = iota((1, taps), 1)
    lane_tile, lane_k = lane // kmax, lane % kmax
    ranks = jnp.zeros((1, taps), jnp.int32)
    for t in range(TILE_ROWS * TILE_COLS):
        ranks = jnp.where(lane_tile == t, rank_ref[t], ranks)
    keep = (lane_tile % TILE_COLS == iota((wide, taps), 0) // nvec) & (lane_k < ranks)
    tall = TILE_ROWS * nvec
    fold = (iota((tall, wide), 0) % nvec == iota((tall, wide), 1) % nvec).astype(BF16)
    own_row = lane_tile // TILE_COLS == iota((tall, taps), 0) // nvec
    row_leaves = cols * points // leaf
    near_rows = iota((row_leaves * nvec, leaf), 0)

    ext[...] = jnp.zeros_like(ext)
    coef[...] = jnp.zeros_like(coef)
    scale[...] = jnp.zeros_like(scale)

    def apart(dr, dc):
        rr, cc = mirrored(r, dr, rows), mirrored(c, dc, cols)
        return rr * cols + cc, {"row": rr, "col": cc}

    def exchange_meta():
        for dr, dc in all_order:
            number, where = apart(dr, dc)
            pltpu.make_async_remote_copy(
                src_ref=msend.at[number], dst_ref=rm.at[dr * cols + c],
                send_sem=m_sem.at[0], recv_sem=m_sem.at[1],
                device_id=where, device_id_type=MESH,
            ).start()
        rm[c] = msend[me]

    def exchange_values():
        for dr, dc in all_order:
            number, where = apart(dr, dc)
            pltpu.make_async_remote_copy(
                src_ref=vsend.at[number], dst_ref=rv.at[dr * cols + dc],
                send_sem=v_send.at[0], recv_sem=v_recv.at[dr],
                device_id=where, device_id_type=MESH,
            ).start()

    def values_of(send, recv, first, count):
        held = rv.at[pl.ds(first, count)]
        return pltpu.make_async_remote_copy(
            src_ref=held, dst_ref=held, send_sem=send, recv_sem=recv,
            device_id={"row": turned(r, 1, rows), "col": c}, device_id_type=MESH,
        )

    def settle(ref, first, count, sem):
        done = ref.at[pl.ds(first, count)]
        copy = pltpu.make_async_remote_copy(
            src_ref=done, dst_ref=done, send_sem=sem.at[0], recv_sem=sem.at[1],
            device_id={"row": turned(r, 1, rows), "col": c}, device_id_type=MESH,
        )
        return copy

    def side(n):
        dr, dc = SIDES[n]
        rr, cc = r + dr, c + dc
        ok = (rr >= 0) & (rr < rows) & (cc >= 0) & (cc < cols)
        return ok, {"row": jnp.clip(rr, 0, rows - 1), "col": jnp.clip(cc, 0, cols - 1)}

    def side_copy(pick, send, recv, n, incoming):
        slot = n if incoming else SIDES.index((-SIDES[n][0], -SIDES[n][1]))
        src, dst = pick(n, slot)
        return pltpu.make_async_remote_copy(
            src_ref=src, dst_ref=dst, send_sem=send.at[n], recv_sem=recv.at[slot],
            device_id=side(n)[1], device_id_type=MESH,
        )

    def sides_start(pick, send, recv):
        for n in range(len(SIDES)):
            @pl.when(side(n)[0])
            def _():
                side_copy(pick, send, recv, n, False).start()

    def sides_wait(pick, send, recv):
        for n in range(len(SIDES)):
            @pl.when(side(n)[0])
            def _():
                side_copy(pick, send, recv, n, True).wait_recv()
                side_copy(pick, send, recv, n, False).wait_send()

    def kappa_sides(n, slot):
        return kappa_ref, kb.at[slot]

    def field_sides(n, slot):
        if 0 in SIDES[n]:
            return brick, hb.at[slot]
        return corner.at[n], hc.at[slot]

    def corner_cells(dr, dc):
        far_x = [CX - x if dr > 0 else x + 1 for x in range(CX)]
        far_y = [CY - y if dc > 0 else y + 1 for y in range(CY)]
        return [(x, y) for x in range(CX) for y in range(CY) if far_x[x] + far_y[y] <= 4]

    gathered = settle(xg, 0, rows - 1, ag_sem)
    gathered.wait_recv()
    for load in loads:
        load.wait()
    own_kappa.wait()
    sides_start(kappa_sides, k_send, k_recv)
    per = tile // points
    for s in range(rows):
        b, j = s // per, s % per
        for q in range(subs):
            at = j * points + q * leaf
            x32[nvec * b : nvec * (b + 1), at : at + leaf] = xg[s, q].astype(F32)
    projected = dot_nt(x32[...].astype(BF16), right_ref[...])
    projected = jnp.where(keep, projected, 0.0).astype(BF16)
    spread_out = jnp.dot(fold, projected, preferred_element_type=F32)
    spread_out = jnp.where(own_row, spread_out, 0.0).astype(BF16)
    exchange_meta()
    far_rows = jnp.dot(spread_out, left_ref[...], preferred_element_type=F32)
    near = jnp.zeros((row_leaves * nvec, leaf), F32)
    for l in range(nleaf):
        column = places_ref[1, l]
        held = xg[column // subs, column % subs].astype(F32)
        spread = jnp.where(near_rows % nvec == 0, held[0:1], held[1:2])
        spread = jnp.where(near_rows // nvec == places_ref[0, l], spread, 0.0)
        near += dot_nt(spread.astype(BF16), leaf_ref[l])
    per_tile = tile // leaf
    for j in range(cols):
        sums = []
        for q in range(subs):
            i = j * subs + q
            at = i % per_tile * leaf
            a = i // per_tile
            sums.append(
                far_rows[nvec * a : nvec * (a + 1), at : at + leaf]
                + near[nvec * i : nvec * (i + 1)]
            )
        terms = pieces(jnp.concatenate(sums, axis=1))
        left_side = jnp.concatenate(
            [
                jnp.concatenate(
                    [
                        dest_hot[:, (j * blocks + b) * LANES : (j * blocks + b + 1) * LANES]
                        * jnp.broadcast_to(
                            term[v : v + 1, b * LANES : (b + 1) * LANES].astype(F32),
                            (devices, LANES),
                        ).astype(BF16)
                        for b in range(blocks)
                    ],
                    axis=1,
                )
                for term in terms
                for v in range(nvec)
            ],
            axis=0,
        )
        packed = dot_nt(left_side, slot_hot[:, j * points : (j + 1) * points])
        packed = packed[: nvec * devices] + packed[nvec * devices :]
        for v in range(nvec):
            vsend[:, j * nvec + v, :] = packed[v * devices : (v + 1) * devices]
    exchange_values()
    sides_wait(kappa_sides, k_send, k_recv)
    strip = 4 * CY

    def laid(ref, get, every):
        for n, (dr, dc) in enumerate(every):
            value = get(dr, dc)
            for x in range(CX):
                at_row = ((dr + 1) * CX + x) * strip + (dc + 1) * CY
                ref[at_row : at_row + CY, :] = value[x * CY : (x + 1) * CY, :]

    every = SIDES + [(0, 0)]

    def valid(dr, dc):
        return (r + dr >= 0) & (r + dr < rows) & (c + dc >= 0) & (c + dc < cols)

    def stiffness(dr, dc):
        if (dr, dc) == (0, 0):
            return (6.0 + kappa_ref[...]) * 0.125
        return jnp.where(valid(dr, dc), (6.0 + kb[SIDES.index((dr, dc))]) * 0.125, 0.0)

    laid(coef, stiffness, every)
    laid(
        scale,
        lambda dr, dc: jnp.full((cells, LANES), jnp.where(valid(dr, dc), 0.125, 0.0), F32),
        every,
    )
    metas = settle(rm, 1, devices - 1, m_sem)
    metas.wait_recv()
    cell_rows = iota((cells, LANES), 0).astype(F32)
    for s in range(devices):
        lane_hot[:, s * LANES : (s + 1) * LANES] = (rm[s, 1:2, :] == lane_rows).astype(BF16)
        hit_hot[:, s * LANES : (s + 1) * LANES] = (rm[s, 0:1, :] == cell_rows).astype(BF16)
    field = jnp.zeros((2 * nvec * cells, LANES), F32)
    for dr in range(rows):
        first = 0 if dr else 1
        values_of(v_send.at[0], v_recv.at[dr], dr * cols + first, cols - first).wait_recv()
        total = rv[dr * cols] if dr else vsend[me]
        for dc in range(1, cols):
            total = total + rv[dr * cols + dc]
        placed = [
            jnp.concatenate(
                [
                    hit_hot[:, (dr * cols + j) * LANES : (dr * cols + j + 1) * LANES]
                    * jnp.broadcast_to(
                        term[j * nvec + v : j * nvec + v + 1, :].astype(F32), (cells, LANES)
                    ).astype(BF16)
                    for j in range(cols)
                ],
                axis=1,
            )
            for term in pieces(total)
            for v in range(nvec)
        ]
        span = slice(dr * cols * LANES, (dr + 1) * cols * LANES)
        field += dot_nt(jnp.concatenate(placed, axis=0), lane_hot[:, span])
    field = field[: nvec * cells] + field[nvec * cells :]
    for v in range(nvec):
        brick[v] = field[v * cells : (v + 1) * cells]
    corners = [n for n in range(len(SIDES)) if 0 not in SIDES[n]]
    for n in corners:
        held = corner_cells(*SIDES[n])
        for v in range(nvec):
            for i, (x, y) in enumerate(held):
                j, cell = v * len(held) + i, v * cells + x * CY + y
                corner[n, j // 4, j % 4 : j % 4 + 1, :] = field[cell : cell + 1]
    sides_start(field_sides, h_send, h_recv)
    gathered.wait_send()
    metas.wait_send()
    values_of(v_send.at[0], v_recv.at[0], 1, devices - 1).wait_send()
    sides_wait(field_sides, h_send, h_recv)

    def bricks(v, dr, dc):
        if (dr, dc) == (0, 0):
            return brick[v]
        return jnp.where(valid(dr, dc), hb[SIDES.index((dr, dc)), v], 0.0)

    for v in range(nvec):
        laid(
            ext.at[v],
            functools.partial(bricks, v),
            [near_side for near_side in every if 0 in near_side],
        )
        for n in corners:
            dr, dc = SIDES[n]
            held = corner_cells(-dr, -dc)
            for i, (x, y) in enumerate(held):
                j = v * len(held) + i
                at_row = ((dr + 1) * CX + x) * strip + (dc + 1) * CY + y
                ext[v, at_row : at_row + 1, :] = jnp.where(
                    valid(dr, dc), hc[n, j // 4, j % 4 : j % 4 + 1, :], 0.0
                )
        cur = ext[v]
        for step in range(4):
            mid = cur[strip:-strip]
            z = iota(mid.shape, 1)
            beside = cur[2 * strip :] + cur[: -2 * strip]
            beside += pltpu.roll(mid, 1, 0) + pltpu.roll(mid, mid.shape[0] - 1, 0)
            beside += jnp.where(z > 0, pltpu.roll(mid, 1, 1), 0.0)
            beside += jnp.where(z < LANES - 1, pltpu.roll(mid, LANES - 1, 1), 0.0)
            low = (step + 1) * strip
            span = slice(low, ext.shape[1] - low)
            cur = coef[span, :] * mid - scale[span, :] * beside
        out_ref[v] = cur.reshape(CX, strip, LANES)


def per_device(
    vectors, lr_left, lr_right, tile_rank, leaf_values, leaf_places, cluster_perm, kappa
):
    rows, cols = lax.axis_size("row"), lax.axis_size("col")
    devices = rows * cols
    nvec, _, points = vectors.shape
    tiles, kmax, tile = lr_left.shape[2:]
    nleaf, leaf = leaf_values.shape[2:4]
    cells, lanes = CX * CY, kappa.shape[2]
    taps = tiles * kmax
    strip, deep = 4 * CY, 3 * CX * 4 * CY
    vmem = pl.BlockSpec(memory_space=pltpu.VMEM)
    hbm = pl.BlockSpec(memory_space=pl.ANY)
    dma = pltpu.SemaphoreType.DMA
    out = pl.pallas_call(
        functools.partial(kernel, rows, cols, kmax, leaf),
        out_shape=pltpu.VMEM((nvec, CX, strip, lanes), F32),
        in_specs=[hbm] * 8,
        out_specs=vmem,
        scratch_shapes=[
            pltpu.SMEM((tiles,), jnp.int32),
            pltpu.SMEM((2, nleaf), jnp.int32),
            pltpu.VMEM((len(SIDES), 3 * nvec // 2, 4, lanes), F32),
            pltpu.VMEM((len(SIDES), 3 * nvec // 2, 4, lanes), F32),
            pltpu.VMEM((cols * points // LANES, LANES), jnp.int32),
            pltpu.VMEM((cells, lanes), F32),
            pltpu.VMEM((taps, tile), BF16),
            pltpu.VMEM((taps, tile), BF16),
            pltpu.VMEM((nleaf, leaf, leaf), BF16),
            pltpu.VMEM((rows, points // leaf, nvec, leaf), BF16),
            pltpu.VMEM((TILE_COLS * nvec, tile), F32),
            pltpu.VMEM((LANES, cols * points), BF16),
            pltpu.VMEM((devices, cols * points), BF16),
            pltpu.VMEM((devices, 2, LANES), F32),
            pltpu.VMEM((devices, 2, LANES), F32),
            pltpu.VMEM((devices, cols * nvec, LANES), F32),
            pltpu.VMEM((devices, cols * nvec, LANES), F32),
            pltpu.VMEM((LANES, devices * LANES), BF16),
            pltpu.VMEM((cells, devices * LANES), BF16),
            pltpu.VMEM((nvec, cells, lanes), F32),
            pltpu.VMEM((len(SIDES), nvec, cells, lanes), F32),
            pltpu.VMEM((len(SIDES), cells, lanes), F32),
            pltpu.VMEM((nvec, deep, lanes), F32),
            pltpu.VMEM((deep, lanes), F32),
            pltpu.VMEM((deep, lanes), F32),
            dma((8,)), dma((2,)), dma((2,)), dma((1,)), dma((rows,)),
            dma((len(SIDES),)), dma((len(SIDES),)), dma((len(SIDES),)), dma((len(SIDES),)),
        ],
        compiler_params=pltpu.CompilerParams(collective_id=0, has_side_effects=True),
    )(
        vectors.reshape(nvec, points // leaf, leaf).transpose(1, 0, 2),
        lr_right.reshape(taps, tile),
        lr_left.reshape(taps, tile),
        tile_rank.reshape(tiles),
        leaf_values.reshape(nleaf, leaf, leaf),
        leaf_places.reshape(nleaf, 2).T,
        cluster_perm.reshape(-1, LANES),
        kappa.reshape(cells, lanes),
    )
    return out[:, :, CY : 2 * CY, :]


def solution(mesh):
    in_specs = (
        P(None, "col", "row"),
        P("row", "col", None, None, None),
        P("row", "col", None, None, None),
        P("row", "col", None),
        P("row", "col", None, None, None),
        P("row", "col", None, None),
        P("row", None),
        P("row", "col", None),
    )
    out_specs = P(None, "row", "col", None)
    return jax.shard_map(
        per_device, mesh=mesh, in_specs=in_specs, out_specs=out_specs, check_vma=False
    )
```

```python
import functools

import jax
import jax.numpy as jnp
from jax import lax
from jax.experimental import pallas as pl
from jax.experimental.pallas import tpu as pltpu
from jax.sharding import PartitionSpec as P

CX = 4
CY = 4
TILE_ROWS = 4
TILE_COLS = 8
LANES = 128
MESH = pl.DeviceIdType.MESH
F32 = jnp.float32
BF16 = jnp.bfloat16
NT = (((1,), (1,)), ((), ()))
SIDES = [(-1, -1), (-1, 1), (1, -1), (1, 1), (0, -1), (0, 1), (-1, 0), (1, 0)]


def dot_nt(a, b):
    return lax.dot_general(a, b, NT, preferred_element_type=F32)


def pieces(x):
    first = x.astype(BF16)
    return first, (x - first.astype(F32)).astype(BF16)


def iota(shape, dim):
    return lax.broadcasted_iota(jnp.int32, shape, dim)


def kernel(
    rows, cols, kmax, leaf,
    x_hbm, right_hbm, left_hbm, rank_hbm, leaf_hbm, places_hbm, perm_hbm, kappa_hbm,
    out_ref,
    rank_ref, places_ref, corner, hc, perm_ref, kappa_ref, right_ref, left_ref, leaf_ref, xg, x32, slot_hot, dest_hot,
    msend, rm, vsend, rv, lane_hot, hit_hot, brick, hb, kb, ext, coef, scale,
    local_sem, ag_send, ag_recv, m_sem, v_send, v_recv, k_send, k_recv, h_send, h_recv,
):
    subs, nvec = x_hbm.shape[:2]
    points = subs * leaf
    tile = right_ref.shape[-1]
    devices = rows * cols
    nleaf = leaf_ref.shape[0]
    cells = CX * CY
    blocks = points // LANES
    r = lax.axis_index("row")
    c = lax.axis_index("col")
    me = r * cols + c

    own_x = pltpu.make_async_copy(x_hbm, xg.at[r], local_sem.at[3])
    own_perm = pltpu.make_async_copy(perm_hbm, perm_ref, local_sem.at[4])
    own_kappa = pltpu.make_async_copy(kappa_hbm, kappa_ref, local_sem.at[5])
    small = [
        pltpu.make_async_copy(rank_hbm, rank_ref, local_sem.at[6]),
        pltpu.make_async_copy(places_hbm, places_ref, local_sem.at[7]),
    ]
    loads = [
        pltpu.make_async_copy(right_hbm, right_ref, local_sem.at[0]),
        pltpu.make_async_copy(left_hbm, left_ref, local_sem.at[1]),
        pltpu.make_async_copy(leaf_hbm, leaf_ref, local_sem.at[2]),
    ]

    def turned(place, by, count):
        moved = place + by
        return moved - jnp.where(moved >= count, count, 0)

    def mirrored(place, by, count):
        if count & (count - 1):
            return turned(place, by, count)
        moved, bit = place, 1
        while bit <= by:
            if by & bit:
                moved = moved + bit - 2 * bit * (place // bit % 2)
            bit *= 2
        return moved

    def far(by):
        return bin(by).count("1")

    row_order = sorted(range(1, rows), key=lambda k: -k)
    col_order = sorted(range(1, cols), key=lambda k: -far(k))
    all_order = sorted(
        ((dr, dc) for dr in range(rows) for dc in range(cols) if dr + dc),
        key=lambda d: -(d[0] // 2 + far(d[1]) + 0.5 * (d[0] % 2)),
    )

    barrier = pltpu.get_barrier_semaphore()
    for k in row_order:
        pl.semaphore_signal(
            barrier, inc=1, device_id={"row": mirrored(r, k, rows), "col": c}, device_id_type=MESH
        )
    for k in col_order:
        pl.semaphore_signal(
            barrier, inc=1, device_id={"row": r, "col": mirrored(c, k, cols)}, device_id_type=MESH
        )
    for load in [own_x, own_perm] + small + [own_kappa] + loads:
        load.start()
    own_x.wait()
    pl.semaphore_wait(barrier, rows + cols - 2)
    for k in row_order:
        pltpu.make_async_remote_copy(
            src_ref=xg.at[r], dst_ref=xg.at[r], send_sem=ag_send.at[0], recv_sem=ag_recv.at[k],
            device_id={"row": mirrored(r, k, rows), "col": c}, device_id_type=MESH,
        ).start()

    own_perm.wait()
    dev_ids = iota((devices, LANES), 0)
    lane_rows = iota((LANES, LANES), 0).astype(F32)
    ahead = (iota((LANES, 2 * LANES), 0) < iota((LANES, 2 * LANES), 1)).astype(BF16)
    for j in range(cols):
        dev_of = perm_ref[j * blocks : (j + 1) * blocks, :] // points
        hots = [(dev_of[b : b + 1, :] == dev_ids).astype(F32) for b in range(blocks)]
        all_hot = jnp.concatenate(hots, axis=0).astype(BF16)
        counts = jnp.dot(all_hot, ahead, preferred_element_type=F32)
        offset = jnp.zeros((devices, LANES), F32)
        for b in range(blocks):
            span = slice(b * devices, (b + 1) * devices)
            at = (j * blocks + b) * LANES
            rank = jnp.sum(hots[b] * (counts[span, :LANES] + offset), axis=0, keepdims=True)
            offset = offset + counts[span, LANES:]
            slot_hot[:, at : at + LANES] = (rank == lane_rows).astype(BF16)
            dest_hot[:, at : at + LANES] = all_hot[span]
    mine = pl.ds(pl.multiple_of(c * points, LANES), points)
    place = perm_ref[pl.ds(pl.multiple_of(c * blocks, 8), blocks), :] % points
    halves = ((place // LANES).astype(F32), (place % LANES).astype(F32))
    dest_mine = dest_hot[:, mine]
    meta = jnp.concatenate(
        [
            jnp.concatenate(
                [
                    dest_mine[:, b * LANES : (b + 1) * LANES]
                    * jnp.broadcast_to(half[b : b + 1, :], (devices, LANES)).astype(BF16)
                    for b in range(blocks)
                ],
                axis=1,
            )
            for half in halves
        ],
        axis=0,
    )
    meta = dot_nt(meta, slot_hot[:, mine])
    for h in range(2):
        msend[:, h, :] = meta[h * devices : (h + 1) * devices]
    for load in small:
        load.wait()
    ext[...] = jnp.zeros_like(ext)
    coef[...] = jnp.zeros_like(coef)
    scale[...] = jnp.zeros_like(scale)
    row_leaves = cols * points // leaf
    near_rows = iota((row_leaves * nvec, leaf), 0)

    ext[...] = jnp.zeros_like(ext)
    coef[...] = jnp.zeros_like(coef)
    scale[...] = jnp.zeros_like(scale)

    def apart(dr, dc):
        rr, cc = mirrored(r, dr, rows), mirrored(c, dc, cols)
        return rr * cols + cc, {"row": rr, "col": cc}

    def exchange_meta():
        for dr, dc in all_order:
            number, where = apart(dr, dc)
            pltpu.make_async_remote_copy(
                src_ref=msend.at[number], dst_ref=rm.at[dr * cols + c],
                send_sem=m_sem.at[0], recv_sem=m_sem.at[1],
                device_id=where, device_id_type=MESH,
            ).start()
        rm[c] = msend[me]

    def exchange_values():
        for dr, dc in all_order:
            number, where = apart(dr, dc)
            pltpu.make_async_remote_copy(
                src_ref=vsend.at[number], dst_ref=rv.at[dr * cols + dc],
                send_sem=v_send.at[0], recv_sem=v_recv.at[dr],
                device_id=where, device_id_type=MESH,
            ).start()

    def values_of(send, recv, first, count):
        held = rv.at[pl.ds(first, count)]
        return pltpu.make_async_remote_copy(
            src_ref=held, dst_ref=held, send_sem=send, recv_sem=recv,
            device_id={"row": turned(r, 1, rows), "col": c}, device_id_type=MESH,
        )

    def settle(ref, first, count, sem):
        done = ref.at[pl.ds(first, count)]
        copy = pltpu.make_async_remote_copy(
            src_ref=done, dst_ref=done, send_sem=sem.at[0], recv_sem=sem.at[1],
            device_id={"row": turned(r, 1, rows), "col": c}, device_id_type=MESH,
        )
        return copy

    def side(n):
        dr, dc = SIDES[n]
        rr, cc = r + dr, c + dc
        ok = (rr >= 0) & (rr < rows) & (cc >= 0) & (cc < cols)
        return ok, {"row": jnp.clip(rr, 0, rows - 1), "col": jnp.clip(cc, 0, cols - 1)}

    def side_copy(pick, send, recv, n, incoming):
        slot = n if incoming else SIDES.index((-SIDES[n][0], -SIDES[n][1]))
        src, dst = pick(n, slot)
        return pltpu.make_async_remote_copy(
            src_ref=src, dst_ref=dst, send_sem=send.at[n], recv_sem=recv.at[slot],
            device_id=side(n)[1], device_id_type=MESH,
        )

    def sides_start(pick, send, recv):
        for n in range(len(SIDES)):
            @pl.when(side(n)[0])
            def _():
                side_copy(pick, send, recv, n, False).start()

    def sides_wait(pick, send, recv):
        for n in range(len(SIDES)):
            @pl.when(side(n)[0])
            def _():
                side_copy(pick, send, recv, n, True).wait_recv()
                side_copy(pick, send, recv, n, False).wait_send()

    def kappa_sides(n, slot):
        return kappa_ref, kb.at[slot]

    def field_sides(n, slot):
        if 0 in SIDES[n]:
            return brick, hb.at[slot]
        return corner.at[n], hc.at[slot]

    def corner_cells(dr, dc):
        far_x = [CX - x if dr > 0 else x + 1 for x in range(CX)]
        far_y = [CY - y if dc > 0 else y + 1 for y in range(CY)]
        return [(x, y) for x in range(CX) for y in range(CY) if far_x[x] + far_y[y] <= 4]

    for load in loads[:2]:
        load.wait()
    per = tile // points
    taps = TILE_ROWS * kmax
    tall = TILE_ROWS * nvec
    groups = rows // per
    stages = [range(groups // 2), range(groups // 2, groups)]

    def columns(g):
        return mirrored(r // per, g, groups)

    def limits(stage):
        lane = iota((1, len(stage) * taps), 1)
        most = jnp.zeros((1, len(stage) * taps), jnp.int32)
        for i, g in enumerate(stage):
            for a in range(TILE_ROWS):
                ours = lane // kmax == i * TILE_ROWS + a
                most = jnp.where(ours, rank_ref[a * TILE_COLS + columns(g)], most)
        return lane % kmax < most

    within = [limits(stage) for stage in stages]

    def arrive(stage):
        for g in stage:
            for k in range(g * per, (g + 1) * per):
                if k:
                    s = mirrored(r, k, rows)
                    pltpu.make_async_remote_copy(
                        src_ref=xg.at[s], dst_ref=xg.at[s], send_sem=ag_send.at[0],
                        recv_sem=ag_recv.at[k], device_id={"row": s, "col": c},
                        device_id_type=MESH,
                    ).wait_recv()

    def project(stage, kept):
        high = len(stage) * nvec
        for g in stage:
            for j in range(per):
                for q in range(subs):
                    at = j * points + q * leaf
                    x32[nvec * g : nvec * (g + 1), at : at + leaf] = xg[
                        columns(g) * per + j, q
                    ].astype(F32)
        right = jnp.concatenate(
            [right_ref[:, columns(g)].reshape(taps, tile) for g in stage], axis=0
        )
        x_rows = x32[nvec * stage[0] : nvec * (stage[-1] + 1), :].astype(BF16)
        seen = dot_nt(x_rows, right)
        row, lane = iota(seen.shape, 0), iota(seen.shape, 1)
        seen = jnp.where((row // nvec == lane // taps) & kept, seen, 0.0)
        part, lane = iota((tall, seen.shape[1]), 0), iota((tall, seen.shape[1]), 1)
        spread = jnp.zeros(part.shape, F32)
        for v in range(nvec):
            ours = jnp.sum(jnp.where(row % nvec == v, seen, 0.0), axis=0, keepdims=True)
            spread = jnp.where(part % nvec == v, ours, spread)
        spread = jnp.where(lane % taps // kmax == part // nvec, spread, 0.0)
        return spread.astype(BF16)

    def expand(stage, spread):
        left = jnp.concatenate(
            [left_ref[:, columns(g)].reshape(taps, tile) for g in stage], axis=0
        )
        return jnp.dot(spread, left, preferred_element_type=F32)

    arrive(stages[0])
    far_rows = expand(stages[0], project(stages[0], within[0]))
    loads[2].wait()
    own_kappa.wait()
    arrive(stages[1])
    exchange_meta()
    sides_start(kappa_sides, k_send, k_recv)
    late = project(stages[1], within[1])
    halves = 2
    side_len = leaf // halves
    straight = [jnp.zeros((row_leaves * nvec, side_len), F32) for _ in range(halves)]
    turned_near = [jnp.zeros((side_len, row_leaves * nvec), F32) for _ in range(halves)]

    def picked(l):
        column = places_ref[1, l]
        held = xg[column // subs, column % subs].astype(F32)
        spread = jnp.where(near_rows % nvec == 0, held[0:1], held[1:2])
        return jnp.where(near_rows // nvec == places_ref[0, l], spread, 0.0).astype(BF16)

    for l in range(0, nleaf, 2):
        flat, tall_x = picked(l), picked(l + 1)
        for k in range(halves):
            deep = slice(k * side_len, (k + 1) * side_len)
            for h in range(halves):
                wide = slice(h * side_len, (h + 1) * side_len)
                turned_near[h] += dot_nt(leaf_ref[l, wide, deep], flat[:, deep])
            for h in range(halves):
                wide = slice(h * side_len, (h + 1) * side_len)
                straight[h] += dot_nt(tall_x[:, deep], leaf_ref[l + 1, wide, deep])
        if l == nleaf // 2:
            far_rows += expand(stages[1], late)
    near = jnp.concatenate(straight, axis=1)
    near += jnp.concatenate(turned_near, axis=0).T
    per_tile = tile // leaf
    for j in range(cols):
        sums = []
        for q in range(subs):
            i = j * subs + q
            at = i % per_tile * leaf
            a = i // per_tile
            sums.append(
                far_rows[nvec * a : nvec * (a + 1), at : at + leaf]
                + near[nvec * i : nvec * (i + 1)]
            )
        terms = pieces(jnp.concatenate(sums, axis=1))
        left_side = jnp.concatenate(
            [
                jnp.concatenate(
                    [
                        dest_hot[:, (j * blocks + b) * LANES : (j * blocks + b + 1) * LANES]
                        * jnp.broadcast_to(
                            term[v : v + 1, b * LANES : (b + 1) * LANES].astype(F32),
                            (devices, LANES),
                        ).astype(BF16)
                        for b in range(blocks)
                    ],
                    axis=1,
                )
                for term in terms
                for v in range(nvec)
            ],
            axis=0,
        )
        packed = dot_nt(left_side, slot_hot[:, j * points : (j + 1) * points])
        packed = packed[: nvec * devices] + packed[nvec * devices :]
        for v in range(nvec):
            vsend[:, j * nvec + v, :] = packed[v * devices : (v + 1) * devices]
    exchange_values()
    sides_wait(kappa_sides, k_send, k_recv)
    strip = 4 * CY

    def laid(ref, get, every):
        for n, (dr, dc) in enumerate(every):
            value = get(dr, dc)
            for x in range(CX):
                at_row = ((dr + 1) * CX + x) * strip + (dc + 1) * CY
                ref[at_row : at_row + CY, :] = value[x * CY : (x + 1) * CY, :]

    every = SIDES + [(0, 0)]

    def valid(dr, dc):
        return (r + dr >= 0) & (r + dr < rows) & (c + dc >= 0) & (c + dc < cols)

    def stiffness(dr, dc):
        if (dr, dc) == (0, 0):
            return (6.0 + kappa_ref[...]) * 0.125
        return jnp.where(valid(dr, dc), (6.0 + kb[SIDES.index((dr, dc))]) * 0.125, 0.0)

    laid(coef, stiffness, every)
    laid(
        scale,
        lambda dr, dc: jnp.full((cells, LANES), jnp.where(valid(dr, dc), 0.125, 0.0), F32),
        every,
    )
    metas = settle(rm, 1, devices - 1, m_sem)
    metas.wait_recv()
    cell_rows = iota((cells, LANES), 0).astype(F32)
    for s in range(devices):
        lane_hot[:, s * LANES : (s + 1) * LANES] = (rm[s, 1:2, :] == lane_rows).astype(BF16)
        hit_hot[:, s * LANES : (s + 1) * LANES] = (rm[s, 0:1, :] == cell_rows).astype(BF16)
    field = jnp.zeros((2 * nvec * cells, LANES), F32)
    for dr in range(rows):
        first = 0 if dr else 1
        values_of(v_send.at[0], v_recv.at[dr], dr * cols + first, cols - first).wait_recv()
        total = rv[dr * cols] if dr else vsend[me]
        for dc in range(1, cols):
            total = total + rv[dr * cols + dc]
        placed = [
            jnp.concatenate(
                [
                    hit_hot[:, (dr * cols + j) * LANES : (dr * cols + j + 1) * LANES]
                    * jnp.broadcast_to(
                        term[j * nvec + v : j * nvec + v + 1, :].astype(F32), (cells, LANES)
                    ).astype(BF16)
                    for j in range(cols)
                ],
                axis=1,
            )
            for term in pieces(total)
            for v in range(nvec)
        ]
        span = slice(dr * cols * LANES, (dr + 1) * cols * LANES)
        field += dot_nt(jnp.concatenate(placed, axis=0), lane_hot[:, span])
    field = field[: nvec * cells] + field[nvec * cells :]
    for v in range(nvec):
        brick[v] = field[v * cells : (v + 1) * cells]
    corners = [n for n in range(len(SIDES)) if 0 not in SIDES[n]]
    for n in corners:
        held = corner_cells(*SIDES[n])
        for v in range(nvec):
            for i, (x, y) in enumerate(held):
                j, cell = v * len(held) + i, v * cells + x * CY + y
                corner[n, j // 4, j % 4 : j % 4 + 1, :] = field[cell : cell + 1]
    sides_start(field_sides, h_send, h_recv)
    rest = xg.at[pl.ds(0, rows - 1)]
    pltpu.make_async_remote_copy(
        src_ref=rest, dst_ref=rest, send_sem=ag_send.at[0], recv_sem=ag_recv.at[0],
        device_id={"row": mirrored(r, 1, rows), "col": c}, device_id_type=MESH,
    ).wait_send()
    metas.wait_send()
    values_of(v_send.at[0], v_recv.at[0], 1, devices - 1).wait_send()
    sides_wait(field_sides, h_send, h_recv)

    def bricks(v, dr, dc):
        if (dr, dc) == (0, 0):
            return brick[v]
        return jnp.where(valid(dr, dc), hb[SIDES.index((dr, dc)), v], 0.0)

    for v in range(nvec):
        laid(
            ext.at[v],
            functools.partial(bricks, v),
            [near_side for near_side in every if 0 in near_side],
        )
        for n in corners:
            dr, dc = SIDES[n]
            held = corner_cells(-dr, -dc)
            for i, (x, y) in enumerate(held):
                j = v * len(held) + i
                at_row = ((dr + 1) * CX + x) * strip + (dc + 1) * CY + y
                ext[v, at_row : at_row + 1, :] = jnp.where(
                    valid(dr, dc), hc[n, j // 4, j % 4 : j % 4 + 1, :], 0.0
                )
        cur = ext[v]
        for step in range(4):
            mid = cur[strip:-strip]
            z = iota(mid.shape, 1)
            beside = cur[2 * strip :] + cur[: -2 * strip]
            beside += pltpu.roll(mid, 1, 0) + pltpu.roll(mid, mid.shape[0] - 1, 0)
            beside += jnp.where(z > 0, pltpu.roll(mid, 1, 1), 0.0)
            beside += jnp.where(z < LANES - 1, pltpu.roll(mid, LANES - 1, 1), 0.0)
            low = (step + 1) * strip
            span = slice(low, ext.shape[1] - low)
            cur = coef[span, :] * mid - scale[span, :] * beside
        out_ref[v] = cur.reshape(CX, strip, LANES)


def per_device(
    vectors, lr_left, lr_right, tile_rank, leaf_values, leaf_places, cluster_perm, kappa
):
    rows, cols = lax.axis_size("row"), lax.axis_size("col")
    devices = rows * cols
    nvec, _, points = vectors.shape
    tiles, kmax, tile = lr_left.shape[2:]
    nleaf, leaf = leaf_values.shape[2:4]
    cells, lanes = CX * CY, kappa.shape[2]
    strip, deep = 4 * CY, 3 * CX * 4 * CY
    vmem = pl.BlockSpec(memory_space=pltpu.VMEM)
    hbm = pl.BlockSpec(memory_space=pl.ANY)
    dma = pltpu.SemaphoreType.DMA
    out = pl.pallas_call(
        functools.partial(kernel, rows, cols, kmax, leaf),
        out_shape=pltpu.VMEM((nvec, CX, strip, lanes), F32),
        in_specs=[hbm] * 8,
        out_specs=vmem,
        scratch_shapes=[
            pltpu.SMEM((tiles,), jnp.int32),
            pltpu.SMEM((2, nleaf), jnp.int32),
            pltpu.VMEM((len(SIDES), 3 * nvec // 2, 4, lanes), F32),
            pltpu.VMEM((len(SIDES), 3 * nvec // 2, 4, lanes), F32),
            pltpu.VMEM((cols * points // LANES, LANES), jnp.int32),
            pltpu.VMEM((cells, lanes), F32),
            pltpu.VMEM((TILE_ROWS, TILE_COLS, kmax, tile), BF16),
            pltpu.VMEM((TILE_ROWS, TILE_COLS, kmax, tile), BF16),
            pltpu.VMEM((nleaf, leaf, leaf), BF16),
            pltpu.VMEM((rows, points // leaf, nvec, leaf), BF16),
            pltpu.VMEM((TILE_COLS * nvec, tile), F32),
            pltpu.VMEM((LANES, cols * points), BF16),
            pltpu.VMEM((devices, cols * points), BF16),
            pltpu.VMEM((devices, 2, LANES), F32),
            pltpu.VMEM((devices, 2, LANES), F32),
            pltpu.VMEM((devices, cols * nvec, LANES), F32),
            pltpu.VMEM((devices, cols * nvec, LANES), F32),
            pltpu.VMEM((LANES, devices * LANES), BF16),
            pltpu.VMEM((cells, devices * LANES), BF16),
            pltpu.VMEM((nvec, cells, lanes), F32),
            pltpu.VMEM((len(SIDES), nvec, cells, lanes), F32),
            pltpu.VMEM((len(SIDES), cells, lanes), F32),
            pltpu.VMEM((nvec, deep, lanes), F32),
            pltpu.VMEM((deep, lanes), F32),
            pltpu.VMEM((deep, lanes), F32),
            dma((8,)), dma((1,)), dma((rows,)), dma((2,)), dma((1,)), dma((rows,)),
            dma((len(SIDES),)), dma((len(SIDES),)), dma((len(SIDES),)), dma((len(SIDES),)),
        ],
        compiler_params=pltpu.CompilerParams(collective_id=0, has_side_effects=True),
    )(
        vectors.reshape(nvec, points // leaf, leaf).transpose(1, 0, 2),
        lr_right.reshape(TILE_ROWS, TILE_COLS, kmax, tile),
        lr_left.reshape(TILE_ROWS, TILE_COLS, kmax, tile),
        tile_rank.reshape(tiles),
        leaf_values.reshape(nleaf, leaf, leaf),
        leaf_places.reshape(nleaf, 2).T,
        cluster_perm.reshape(-1, LANES),
        kappa.reshape(cells, lanes),
    )
    return out[:, :, CY : 2 * CY, :]


def solution(mesh):
    in_specs = (
        P(None, "col", "row"),
        P("row", "col", None, None, None),
        P("row", "col", None, None, None),
        P("row", "col", None),
        P("row", "col", None, None, None),
        P("row", "col", None, None),
        P("row", None),
        P("row", "col", None),
    )
    out_specs = P(None, "row", "col", None)
    return jax.shard_map(
        per_device, mesh=mesh, in_specs=in_specs, out_specs=out_specs, check_vma=False
    )
```

```python
import functools

import jax
import jax.numpy as jnp
from jax import lax
from jax.experimental import pallas as pl
from jax.experimental.pallas import tpu as pltpu
from jax.sharding import PartitionSpec as P

CX = 4
CY = 4
TILE_ROWS = 4
TILE_COLS = 8
LANES = 128
MESH = pl.DeviceIdType.MESH
F32 = jnp.float32
BF16 = jnp.bfloat16
NT = (((1,), (1,)), ((), ()))
SIDES = [(-1, -1), (-1, 1), (1, -1), (1, 1), (0, -1), (0, 1), (-1, 0), (1, 0)]


def dot_nt(a, b):
    return lax.dot_general(a, b, NT, preferred_element_type=F32)


def pieces(x):
    first = x.astype(BF16)
    return first, (x - first.astype(F32)).astype(BF16)


def iota(shape, dim):
    return lax.broadcasted_iota(jnp.int32, shape, dim)


def kernel(
    rows, cols, kmax, leaf,
    x_hbm, right_hbm, left_hbm, rank_hbm, leaf_hbm, places_hbm, perm_hbm, kappa_hbm,
    out_ref,
    rank_ref, places_ref, corner, hc, perm_ref, kappa_ref, right_ref, left_ref, leaf_ref, xg, x32, slot_hot, dest_hot,
    msend, rm, vsend, rv, lane_hot, hit_hot, brick, hb, kb, ext, work, coef, scale,
    local_sem, ag_send, ag_recv, m_sem, v_send, v_recv, k_send, k_recv, h_send, h_recv,
):
    subs, nvec = x_hbm.shape[:2]
    points = subs * leaf
    tile = right_ref.shape[-1]
    devices = rows * cols
    nleaf = leaf_ref.shape[0]
    cells = CX * CY
    blocks = points // LANES
    r = lax.axis_index("row")
    c = lax.axis_index("col")
    me = r * cols + c

    own_x = pltpu.make_async_copy(x_hbm, xg.at[r], local_sem.at[3])
    own_perm = pltpu.make_async_copy(perm_hbm, perm_ref, local_sem.at[4])
    own_kappa = pltpu.make_async_copy(kappa_hbm, kappa_ref, local_sem.at[5])
    small = [
        pltpu.make_async_copy(rank_hbm, rank_ref, local_sem.at[6]),
        pltpu.make_async_copy(places_hbm, places_ref, local_sem.at[7]),
    ]
    loads = [
        pltpu.make_async_copy(right_hbm, right_ref, local_sem.at[0]),
        pltpu.make_async_copy(left_hbm, left_ref, local_sem.at[1]),
        pltpu.make_async_copy(leaf_hbm, leaf_ref, local_sem.at[2]),
    ]

    def turned(place, by, count):
        moved = place + by
        return moved - jnp.where(moved >= count, count, 0)

    def mirrored(place, by, count):
        if count & (count - 1):
            return turned(place, by, count)
        moved, bit = place, 1
        while bit <= by:
            if by & bit:
                moved = moved + bit - 2 * bit * (place // bit % 2)
            bit *= 2
        return moved

    def far(by):
        return bin(by).count("1")

    row_order = sorted(range(1, rows), key=lambda k: -k)
    col_order = sorted(range(1, cols), key=lambda k: -far(k))
    all_order = sorted(
        ((dr, dc) for dr in range(rows) for dc in range(cols) if dr + dc),
        key=lambda d: -(d[0] // 2 + far(d[1]) + 0.5 * (d[0] % 2)),
    )

    barrier = pltpu.get_barrier_semaphore()
    for k in row_order:
        pl.semaphore_signal(
            barrier, inc=1, device_id={"row": mirrored(r, k, rows), "col": c}, device_id_type=MESH
        )
    for k in col_order:
        pl.semaphore_signal(
            barrier, inc=1, device_id={"row": r, "col": mirrored(c, k, cols)}, device_id_type=MESH
        )
    for load in [own_x, own_perm] + small + [own_kappa] + loads:
        load.start()
    own_x.wait()
    pl.semaphore_wait(barrier, rows + cols - 2)
    for k in row_order:
        pltpu.make_async_remote_copy(
            src_ref=xg.at[r], dst_ref=xg.at[r], send_sem=ag_send.at[0], recv_sem=ag_recv.at[k],
            device_id={"row": mirrored(r, k, rows), "col": c}, device_id_type=MESH,
        ).start()

    own_perm.wait()
    dev_ids = iota((devices, LANES), 0)
    lane_rows = iota((LANES, LANES), 0).astype(F32)
    ahead = (iota((LANES, 2 * LANES), 0) < iota((LANES, 2 * LANES), 1)).astype(BF16)
    for j in range(cols):
        dev_of = perm_ref[j * blocks : (j + 1) * blocks, :] // points
        hots = [(dev_of[b : b + 1, :] == dev_ids).astype(F32) for b in range(blocks)]
        all_hot = jnp.concatenate(hots, axis=0).astype(BF16)
        counts = jnp.dot(all_hot, ahead, preferred_element_type=F32)
        offset = jnp.zeros((devices, LANES), F32)
        for b in range(blocks):
            span = slice(b * devices, (b + 1) * devices)
            at = (j * blocks + b) * LANES
            rank = jnp.sum(hots[b] * (counts[span, :LANES] + offset), axis=0, keepdims=True)
            offset = offset + counts[span, LANES:]
            slot_hot[:, at : at + LANES] = (rank == lane_rows).astype(BF16)
            dest_hot[:, at : at + LANES] = all_hot[span]
    mine = pl.ds(pl.multiple_of(c * points, LANES), points)
    place = perm_ref[pl.ds(pl.multiple_of(c * blocks, 8), blocks), :] % points
    halves = ((place // LANES).astype(F32), (place % LANES).astype(F32))
    dest_mine = dest_hot[:, mine]
    meta = jnp.concatenate(
        [
            jnp.concatenate(
                [
                    dest_mine[:, b * LANES : (b + 1) * LANES]
                    * jnp.broadcast_to(half[b : b + 1, :], (devices, LANES)).astype(BF16)
                    for b in range(blocks)
                ],
                axis=1,
            )
            for half in halves
        ],
        axis=0,
    )
    meta = dot_nt(meta, slot_hot[:, mine])
    for h in range(2):
        msend[:, h, :] = meta[h * devices : (h + 1) * devices]
    for load in small:
        load.wait()
    ext[...] = jnp.zeros_like(ext)
    coef[...] = jnp.zeros_like(coef)
    scale[...] = jnp.zeros_like(scale)
    row_leaves = cols * points // leaf
    near_rows = iota((row_leaves * nvec, leaf), 0)

    ext[...] = jnp.zeros_like(ext)
    coef[...] = jnp.zeros_like(coef)
    scale[...] = jnp.zeros_like(scale)

    def apart(dr, dc):
        rr, cc = mirrored(r, dr, rows), mirrored(c, dc, cols)
        return rr * cols + cc, {"row": rr, "col": cc}

    def send_meta(peers):
        for dr, dc in peers:
            number, where = apart(dr, dc)
            pltpu.make_async_remote_copy(
                src_ref=msend.at[number], dst_ref=rm.at[dr * cols + c],
                send_sem=m_sem.at[0], recv_sem=m_sem.at[1],
                device_id=where, device_id_type=MESH,
            ).start()

    def exchange_values():
        for dr, dc in all_order:
            number, where = apart(dr, dc)
            pltpu.make_async_remote_copy(
                src_ref=vsend.at[number], dst_ref=rv.at[dr * cols + dc],
                send_sem=v_send.at[0], recv_sem=v_recv.at[dr],
                device_id=where, device_id_type=MESH,
            ).start()

    def values_of(send, recv, first, count):
        held = rv.at[pl.ds(first, count)]
        return pltpu.make_async_remote_copy(
            src_ref=held, dst_ref=held, send_sem=send, recv_sem=recv,
            device_id={"row": turned(r, 1, rows), "col": c}, device_id_type=MESH,
        )

    def settle(ref, first, count, sem):
        done = ref.at[pl.ds(first, count)]
        copy = pltpu.make_async_remote_copy(
            src_ref=done, dst_ref=done, send_sem=sem.at[0], recv_sem=sem.at[1],
            device_id={"row": turned(r, 1, rows), "col": c}, device_id_type=MESH,
        )
        return copy

    def side(n):
        dr, dc = SIDES[n]
        rr, cc = r + dr, c + dc
        ok = (rr >= 0) & (rr < rows) & (cc >= 0) & (cc < cols)
        return ok, {"row": jnp.clip(rr, 0, rows - 1), "col": jnp.clip(cc, 0, cols - 1)}

    def side_copy(pick, send, recv, n, incoming):
        slot = n if incoming else SIDES.index((-SIDES[n][0], -SIDES[n][1]))
        src, dst = pick(n, slot)
        return pltpu.make_async_remote_copy(
            src_ref=src, dst_ref=dst, send_sem=send.at[n], recv_sem=recv.at[slot],
            device_id=side(n)[1], device_id_type=MESH,
        )

    def sides_start(pick, send, recv):
        for n in range(len(SIDES)):
            @pl.when(side(n)[0])
            def _():
                side_copy(pick, send, recv, n, False).start()

    def sides_wait(pick, send, recv):
        for n in range(len(SIDES)):
            @pl.when(side(n)[0])
            def _():
                side_copy(pick, send, recv, n, True).wait_recv()
                side_copy(pick, send, recv, n, False).wait_send()

    def kappa_sides(n, slot):
        return kappa_ref, kb.at[slot]

    def field_sides(n, slot):
        if 0 in SIDES[n]:
            return brick, hb.at[slot]
        return corner.at[n], hc.at[slot]

    def corner_cells(dr, dc):
        far_x = [CX - x if dr > 0 else x + 1 for x in range(CX)]
        far_y = [CY - y if dc > 0 else y + 1 for y in range(CY)]
        return [(x, y) for x in range(CX) for y in range(CY) if far_x[x] + far_y[y] <= 4]

    for load in loads[:2]:
        load.wait()
    per = tile // points
    taps = TILE_ROWS * kmax
    tall = TILE_ROWS * nvec
    groups = rows // per
    stages = [range(groups // 2), range(groups // 2, groups)]

    def columns(g):
        return mirrored(r // per, g, groups)

    def limits(stage):
        lane = iota((1, len(stage) * taps), 1)
        most = jnp.zeros((1, len(stage) * taps), jnp.int32)
        for i, g in enumerate(stage):
            for a in range(TILE_ROWS):
                ours = lane // kmax == i * TILE_ROWS + a
                most = jnp.where(ours, rank_ref[a * TILE_COLS + columns(g)], most)
        return lane % kmax < most

    within = [limits(stage) for stage in stages]

    def arrive(stage):
        for g in stage:
            for k in range(g * per, (g + 1) * per):
                if k:
                    s = mirrored(r, k, rows)
                    pltpu.make_async_remote_copy(
                        src_ref=xg.at[s], dst_ref=xg.at[s], send_sem=ag_send.at[0],
                        recv_sem=ag_recv.at[k], device_id={"row": s, "col": c},
                        device_id_type=MESH,
                    ).wait_recv()

    def project(stage, kept):
        high = len(stage) * nvec
        for g in stage:
            for j in range(per):
                for q in range(subs):
                    at = j * points + q * leaf
                    x32[nvec * g : nvec * (g + 1), at : at + leaf] = xg[
                        columns(g) * per + j, q
                    ].astype(F32)
        right = jnp.concatenate(
            [right_ref[:, columns(g)].reshape(taps, tile) for g in stage], axis=0
        )
        x_rows = x32[nvec * stage[0] : nvec * (stage[-1] + 1), :].astype(BF16)
        seen = dot_nt(x_rows, right)
        row, lane = iota(seen.shape, 0), iota(seen.shape, 1)
        seen = jnp.where((row // nvec == lane // taps) & kept, seen, 0.0)
        part, lane = iota((tall, seen.shape[1]), 0), iota((tall, seen.shape[1]), 1)
        spread = jnp.zeros(part.shape, F32)
        for v in range(nvec):
            ours = jnp.sum(jnp.where(row % nvec == v, seen, 0.0), axis=0, keepdims=True)
            spread = jnp.where(part % nvec == v, ours, spread)
        spread = jnp.where(lane % taps // kmax == part // nvec, spread, 0.0)
        return spread.astype(BF16)

    def expand(stage, spread):
        left = jnp.concatenate(
            [left_ref[:, columns(g)].reshape(taps, tile) for g in stage], axis=0
        )
        return jnp.dot(spread, left, preferred_element_type=F32)

    arrive(stages[0])
    met = len(stages[0]) * per
    send_meta([d for d in all_order if d[0] < met])
    rm[c] = msend[me]
    far_rows = expand(stages[0], project(stages[0], within[0]))
    loads[2].wait()
    own_kappa.wait()
    arrive(stages[1])
    later = [d for d in all_order if d[0] >= met]
    late = project(stages[1], within[1])
    halves = 2
    side_len = leaf // halves
    straight = [jnp.zeros((row_leaves * nvec, leaf), F32) for _ in range(halves)]
    turned_near = [jnp.zeros((side_len, row_leaves * nvec), F32) for _ in range(halves)]

    def picked(l):
        column = places_ref[1, l]
        held = xg[column // subs, column % subs].astype(F32)
        spread = jnp.where(near_rows % nvec == 0, held[0:1], held[1:2])
        return jnp.where(near_rows // nvec == places_ref[0, l], spread, 0.0).astype(BF16)

    cuts = [slice(h * side_len, (h + 1) * side_len) for h in range(halves)]
    for l in range(0, nleaf, 2):
        flat, tall_x = picked(l), picked(l + 1)
        turned_near[0] += dot_nt(leaf_ref[l, cuts[0], cuts[0]], flat[:, cuts[0]])
        send_meta(later[:2])
        later = later[2:]
        turned_near[1] += dot_nt(leaf_ref[l, cuts[1], cuts[0]], flat[:, cuts[0]])
        send_meta(later[:2])
        later = later[2:]
        straight[0] += dot_nt(tall_x[:, cuts[0]], leaf_ref[l + 1, :, cuts[0]])
        send_meta(later[:2])
        later = later[2:]
        turned_near[0] += dot_nt(leaf_ref[l, cuts[0], cuts[1]], flat[:, cuts[1]])
        send_meta(later[:2])
        later = later[2:]
        turned_near[1] += dot_nt(leaf_ref[l, cuts[1], cuts[1]], flat[:, cuts[1]])
        send_meta(later[:2])
        later = later[2:]
        straight[1] += dot_nt(tall_x[:, cuts[1]], leaf_ref[l + 1, :, cuts[1]])
        send_meta(later[:2])
        later = later[2:]
        if l == nleaf // 2:
            far_rows += expand(stages[1], late)
    near = straight[0] + straight[1]
    send_meta(later)
    near += jnp.concatenate(turned_near, axis=0).T
    per_tile = tile // leaf
    for j in range(cols):
        sums = []
        for q in range(subs):
            i = j * subs + q
            at = i % per_tile * leaf
            a = i // per_tile
            sums.append(
                far_rows[nvec * a : nvec * (a + 1), at : at + leaf]
                + near[nvec * i : nvec * (i + 1)]
            )
        terms = pieces(jnp.concatenate(sums, axis=1))
        left_side = jnp.concatenate(
            [
                jnp.concatenate(
                    [
                        dest_hot[:, (j * blocks + b) * LANES : (j * blocks + b + 1) * LANES]
                        * jnp.broadcast_to(
                            term[v : v + 1, b * LANES : (b + 1) * LANES].astype(F32),
                            (devices, LANES),
                        ).astype(BF16)
                        for b in range(blocks)
                    ],
                    axis=1,
                )
                for term in terms
                for v in range(nvec)
            ],
            axis=0,
        )
        packed = dot_nt(left_side, slot_hot[:, j * points : (j + 1) * points])
        packed = packed[: nvec * devices] + packed[nvec * devices :]
        for v in range(nvec):
            vsend[:, j * nvec + v, :] = packed[v * devices : (v + 1) * devices]
    exchange_values()
    sides_start(kappa_sides, k_send, k_recv)
    metas = settle(rm, 1, devices - 1, m_sem)
    metas.wait_recv()
    cell_rows = iota((cells, LANES), 0).astype(F32)
    for s in range(devices):
        lane_hot[:, s * LANES : (s + 1) * LANES] = (rm[s, 1:2, :] == lane_rows).astype(BF16)
        hit_hot[:, s * LANES : (s + 1) * LANES] = (rm[s, 0:1, :] == cell_rows).astype(BF16)
    field = jnp.zeros((2 * nvec * cells, LANES), F32)
    for dr in range(rows):
        first = 0 if dr else 1
        values_of(v_send.at[0], v_recv.at[dr], dr * cols + first, cols - first).wait_recv()
        total = rv[dr * cols] if dr else vsend[me]
        for dc in range(1, cols):
            total = total + rv[dr * cols + dc]
        placed = [
            jnp.concatenate(
                [
                    hit_hot[:, (dr * cols + j) * LANES : (dr * cols + j + 1) * LANES]
                    * jnp.broadcast_to(
                        term[j * nvec + v : j * nvec + v + 1, :].astype(F32), (cells, LANES)
                    ).astype(BF16)
                    for j in range(cols)
                ],
                axis=1,
            )
            for term in pieces(total)
            for v in range(nvec)
        ]
        span = slice(dr * cols * LANES, (dr + 1) * cols * LANES)
        field += dot_nt(jnp.concatenate(placed, axis=0), lane_hot[:, span])
    field = field[: nvec * cells] + field[nvec * cells :]
    for v in range(nvec):
        brick[v] = field[v * cells : (v + 1) * cells]
    corners = [n for n in range(len(SIDES)) if 0 not in SIDES[n]]
    for n in corners:
        held = corner_cells(*SIDES[n])
        for v in range(nvec):
            for i, (x, y) in enumerate(held):
                j, cell = v * len(held) + i, v * cells + x * CY + y
                corner[n, j // 4, j % 4 : j % 4 + 1, :] = field[cell : cell + 1]
    sides_start(field_sides, h_send, h_recv)
    rest = xg.at[pl.ds(0, rows - 1)]
    pltpu.make_async_remote_copy(
        src_ref=rest, dst_ref=rest, send_sem=ag_send.at[0], recv_sem=ag_recv.at[0],
        device_id={"row": mirrored(r, 1, rows), "col": c}, device_id_type=MESH,
    ).wait_send()
    metas.wait_send()
    values_of(v_send.at[0], v_recv.at[0], 1, devices - 1).wait_send()
    sides_wait(kappa_sides, k_send, k_recv)
    strip = 4 * CY

    def laid(ref, get, every):
        for n, (dr, dc) in enumerate(every):
            value = get(dr, dc)
            for x in range(CX):
                at_row = ((dr + 1) * CX + x) * strip + (dc + 1) * CY
                ref[at_row : at_row + CY, :] = value[x * CY : (x + 1) * CY, :]

    every = SIDES + [(0, 0)]

    def valid(dr, dc):
        return (r + dr >= 0) & (r + dr < rows) & (c + dc >= 0) & (c + dc < cols)

    def stiffness(dr, dc):
        if (dr, dc) == (0, 0):
            return (6.0 + kappa_ref[...]) * 0.125
        return jnp.where(valid(dr, dc), (6.0 + kb[SIDES.index((dr, dc))]) * 0.125, 0.0)

    laid(coef, stiffness, every)
    laid(
        scale,
        lambda dr, dc: jnp.full((cells, LANES), jnp.where(valid(dr, dc), 0.125, 0.0), F32),
        every,
    )
    sides_wait(field_sides, h_send, h_recv)

    def bricks(v, dr, dc):
        if (dr, dc) == (0, 0):
            return brick[v]
        return jnp.where(valid(dr, dc), hb[SIDES.index((dr, dc)), v], 0.0)

    for v in range(nvec):
        laid(
            ext.at[v],
            functools.partial(bricks, v),
            [near_side for near_side in every if 0 in near_side],
        )
        for n in corners:
            dr, dc = SIDES[n]
            held = corner_cells(-dr, -dc)
            for i, (x, y) in enumerate(held):
                j = v * len(held) + i
                at_row = ((dr + 1) * CX + x) * strip + (dc + 1) * CY + y
                ext[v, at_row : at_row + 1, :] = jnp.where(
                    valid(dr, dc), hc[n, j // 4, j % 4 : j % 4 + 1, :], 0.0
                )
    rows_in = ext.shape[1]
    for step in range(4):
        low = (step + 1) * strip
        count = rows_in - 2 * low
        for v in range(nvec):
            src = ext if step % 2 == 0 else work

            def at(by):
                return src[v, pl.ds(low + by, count), :]

            mid = src[v, low : low + count, :]
            z = iota(mid.shape, 1)
            beside = src[v, low + strip : low + strip + count, :]
            beside += src[v, low - strip : low - strip + count, :]
            beside += at(1) + at(-1)
            beside += jnp.where(z > 0, pltpu.roll(mid, 1, 1), 0.0)
            beside += jnp.where(z < LANES - 1, pltpu.roll(mid, LANES - 1, 1), 0.0)
            span = slice(low, low + count)
            cur = coef[span, :] * mid - scale[span, :] * beside
            if step < 3:
                (work if step % 2 == 0 else ext)[v, span, :] = cur
            else:
                out_ref[v] = cur.reshape(CX, strip, LANES)


def per_device(
    vectors, lr_left, lr_right, tile_rank, leaf_values, leaf_places, cluster_perm, kappa
):
    rows, cols = lax.axis_size("row"), lax.axis_size("col")
    devices = rows * cols
    nvec, _, points = vectors.shape
    tiles, kmax, tile = lr_left.shape[2:]
    nleaf, leaf = leaf_values.shape[2:4]
    cells, lanes = CX * CY, kappa.shape[2]
    strip, deep = 4 * CY, 3 * CX * 4 * CY
    vmem = pl.BlockSpec(memory_space=pltpu.VMEM)
    hbm = pl.BlockSpec(memory_space=pl.ANY)
    dma = pltpu.SemaphoreType.DMA
    out = pl.pallas_call(
        functools.partial(kernel, rows, cols, kmax, leaf),
        out_shape=pltpu.VMEM((nvec, CX, strip, lanes), F32),
        in_specs=[hbm] * 8,
        out_specs=vmem,
        scratch_shapes=[
            pltpu.SMEM((tiles,), jnp.int32),
            pltpu.SMEM((2, nleaf), jnp.int32),
            pltpu.VMEM((len(SIDES), 3 * nvec // 2, 4, lanes), F32),
            pltpu.VMEM((len(SIDES), 3 * nvec // 2, 4, lanes), F32),
            pltpu.VMEM((cols * points // LANES, LANES), jnp.int32),
            pltpu.VMEM((cells, lanes), F32),
            pltpu.VMEM((TILE_ROWS, TILE_COLS, kmax, tile), BF16),
            pltpu.VMEM((TILE_ROWS, TILE_COLS, kmax, tile), BF16),
            pltpu.VMEM((nleaf, leaf, leaf), BF16),
            pltpu.VMEM((rows, points // leaf, nvec, leaf), BF16),
            pltpu.VMEM((TILE_COLS * nvec, tile), F32),
            pltpu.VMEM((LANES, cols * points), BF16),
            pltpu.VMEM((devices, cols * points), BF16),
            pltpu.VMEM((devices, 2, LANES), F32),
            pltpu.VMEM((devices, 2, LANES), F32),
            pltpu.VMEM((devices, cols * nvec, LANES), F32),
            pltpu.VMEM((devices, cols * nvec, LANES), F32),
            pltpu.VMEM((LANES, devices * LANES), BF16),
            pltpu.VMEM((cells, devices * LANES), BF16),
            pltpu.VMEM((nvec, cells, lanes), F32),
            pltpu.VMEM((len(SIDES), nvec, cells, lanes), F32),
            pltpu.VMEM((len(SIDES), cells, lanes), F32),
            pltpu.VMEM((nvec, deep, lanes), F32),
            pltpu.VMEM((nvec, deep, lanes), F32),
            pltpu.VMEM((deep, lanes), F32),
            pltpu.VMEM((deep, lanes), F32),
            dma((8,)), dma((1,)), dma((rows,)), dma((2,)), dma((1,)), dma((rows,)),
            dma((len(SIDES),)), dma((len(SIDES),)), dma((len(SIDES),)), dma((len(SIDES),)),
        ],
        compiler_params=pltpu.CompilerParams(collective_id=0, has_side_effects=True),
    )(
        vectors.reshape(nvec, points // leaf, leaf).transpose(1, 0, 2),
        lr_right.reshape(TILE_ROWS, TILE_COLS, kmax, tile),
        lr_left.reshape(TILE_ROWS, TILE_COLS, kmax, tile),
        tile_rank.reshape(tiles),
        leaf_values.reshape(nleaf, leaf, leaf),
        leaf_places.reshape(nleaf, 2).T,
        cluster_perm.reshape(-1, LANES),
        kappa.reshape(cells, lanes),
    )
    return out[:, :, CY : 2 * CY, :]


def solution(mesh):
    in_specs = (
        P(None, "col", "row"),
        P("row", "col", None, None, None),
        P("row", "col", None, None, None),
        P("row", "col", None),
        P("row", "col", None, None, None),
        P("row", "col", None, None),
        P("row", None),
        P("row", "col", None),
    )
    out_specs = P(None, "row", "col", None)
    return jax.shard_map(
        per_device, mesh=mesh, in_specs=in_specs, out_specs=out_specs, check_vma=False
    )
```

```python
import functools

import jax
import jax.numpy as jnp
from jax import lax
from jax.experimental import pallas as pl
from jax.experimental.pallas import tpu as pltpu
from jax.sharding import PartitionSpec as P

CX = 4
CY = 4
TILE_ROWS = 4
TILE_COLS = 8
LANES = 128
MESH = pl.DeviceIdType.MESH
F32 = jnp.float32
BF16 = jnp.bfloat16
NT = (((1,), (1,)), ((), ()))
SIDES = [(-1, -1), (-1, 1), (1, -1), (1, 1), (0, -1), (0, 1), (-1, 0), (1, 0)]


def dot_nt(a, b):
    return lax.dot_general(a, b, NT, preferred_element_type=F32)


def pieces(x):
    first = x.astype(BF16)
    return first, (x - first.astype(F32)).astype(BF16)


def span_of(grade):
    return jnp.exp2(grade.astype(F32) * 0.125)


def coded(values, grade):
    first, second = (
        jnp.floor(v * (32000.0 / span_of(grade)) + 0.5).astype(jnp.int32) for v in values
    )
    return first * 65536 + second


def decoded(code, grade):
    second = jnp.right_shift(jnp.left_shift(code, 16), 16)
    first = jnp.right_shift(code - second, 16)
    unit = span_of(grade) * (1.0 / 32000.0)
    return first.astype(F32) * unit, second.astype(F32) * unit


def iota(shape, dim):
    return lax.broadcasted_iota(jnp.int32, shape, dim)


def kernel(
    rows, cols, kmax, leaf,
    x_hbm, right_hbm, left_hbm, rank_hbm, leaf_hbm, places_hbm, perm_hbm, kappa_hbm,
    out_ref,
    rank_ref, places_ref, corner, hc, perm_ref, kappa_ref, right_ref, left_ref, leaf_ref, xg, x32, slot_hot, dest_hot,
    msend, rm, vsend, rv, lane_hot, hit_hot, brick, hb, kb, ext, work, coef, scale,
    local_sem, ag_send, ag_recv, m_sem, v_send, v_recv, k_send, k_recv, h_send, h_recv,
):
    subs, nvec = x_hbm.shape[:2]
    points = subs * leaf
    tile = right_ref.shape[-1]
    devices = rows * cols
    nleaf = leaf_ref.shape[0]
    cells = CX * CY
    blocks = points // LANES
    r = lax.axis_index("row")
    c = lax.axis_index("col")
    me = r * cols + c

    own_x = pltpu.make_async_copy(x_hbm, xg.at[r], local_sem.at[3])
    own_perm = pltpu.make_async_copy(perm_hbm, perm_ref, local_sem.at[4])
    own_kappa = pltpu.make_async_copy(kappa_hbm, kappa_ref, local_sem.at[5])
    small = [
        pltpu.make_async_copy(rank_hbm, rank_ref, local_sem.at[6]),
        pltpu.make_async_copy(places_hbm, places_ref, local_sem.at[7]),
    ]
    loads = [
        pltpu.make_async_copy(right_hbm, right_ref, local_sem.at[0]),
        pltpu.make_async_copy(left_hbm, left_ref, local_sem.at[1]),
        pltpu.make_async_copy(leaf_hbm, leaf_ref, local_sem.at[2]),
    ]

    def turned(place, by, count):
        moved = place + by
        return moved - jnp.where(moved >= count, count, 0)

    def mirrored(place, by, count):
        if count & (count - 1):
            return turned(place, by, count)
        moved, bit = place, 1
        while bit <= by:
            if by & bit:
                moved = moved + bit - 2 * bit * (place // bit % 2)
            bit *= 2
        return moved

    def far(by):
        return bin(by).count("1")

    row_order = sorted(range(1, rows), key=lambda k: -k)
    col_order = sorted(range(1, cols), key=lambda k: -far(k))
    all_order = sorted(
        ((dr, dc) for dr in range(rows) for dc in range(cols) if dr + dc),
        key=lambda d: -(d[0] // 2 + far(d[1]) + 0.5 * (d[0] % 2)),
    )

    barrier = pltpu.get_barrier_semaphore()
    for k in row_order:
        pl.semaphore_signal(
            barrier, inc=1, device_id={"row": mirrored(r, k, rows), "col": c}, device_id_type=MESH
        )
    for k in col_order:
        pl.semaphore_signal(
            barrier, inc=1, device_id={"row": r, "col": mirrored(c, k, cols)}, device_id_type=MESH
        )
    for load in [own_x, own_perm] + small + [own_kappa] + loads:
        load.start()
    own_x.wait()
    pl.semaphore_wait(barrier, rows + cols - 2)
    for k in row_order:
        pltpu.make_async_remote_copy(
            src_ref=xg.at[r], dst_ref=xg.at[r], send_sem=ag_send.at[0], recv_sem=ag_recv.at[k],
            device_id={"row": mirrored(r, k, rows), "col": c}, device_id_type=MESH,
        ).start()

    own_perm.wait()
    dev_ids = iota((devices, LANES), 0)
    lane_rows = iota((LANES, LANES), 0).astype(F32)
    ahead = (iota((LANES, 2 * LANES), 0) < iota((LANES, 2 * LANES), 1)).astype(BF16)
    for j in range(cols):
        dev_of = perm_ref[j * blocks : (j + 1) * blocks, :] // points
        hots = [(dev_of[b : b + 1, :] == dev_ids).astype(F32) for b in range(blocks)]
        all_hot = jnp.concatenate(hots, axis=0).astype(BF16)
        counts = jnp.dot(all_hot, ahead, preferred_element_type=F32)
        offset = jnp.zeros((devices, LANES), F32)
        for b in range(blocks):
            span = slice(b * devices, (b + 1) * devices)
            at = (j * blocks + b) * LANES
            rank = jnp.sum(hots[b] * (counts[span, :LANES] + offset), axis=0, keepdims=True)
            offset = offset + counts[span, LANES:]
            slot_hot[:, at : at + LANES] = (rank == lane_rows).astype(BF16)
            dest_hot[:, at : at + LANES] = all_hot[span]
    mine = pl.ds(pl.multiple_of(c * points, LANES), points)
    place = perm_ref[pl.ds(pl.multiple_of(c * blocks, 8), blocks), :] % points
    halves = ((place // LANES).astype(F32), (place % LANES).astype(F32))
    dest_mine = dest_hot[:, mine]
    meta = jnp.concatenate(
        [
            jnp.concatenate(
                [
                    dest_mine[:, b * LANES : (b + 1) * LANES]
                    * jnp.broadcast_to(half[b : b + 1, :], (devices, LANES)).astype(BF16)
                    for b in range(blocks)
                ],
                axis=1,
            )
            for half in halves
        ],
        axis=0,
    )
    meta = dot_nt(meta, slot_hot[:, mine])
    for h in range(2):
        msend[:, h, :] = meta[h * devices : (h + 1) * devices]
    for load in small:
        load.wait()
    ext[...] = jnp.zeros_like(ext)
    coef[...] = jnp.zeros_like(coef)
    scale[...] = jnp.zeros_like(scale)
    row_leaves = cols * points // leaf
    near_rows = iota((row_leaves * nvec, leaf), 0)

    ext[...] = jnp.zeros_like(ext)
    coef[...] = jnp.zeros_like(coef)
    scale[...] = jnp.zeros_like(scale)

    def apart(dr, dc):
        rr, cc = mirrored(r, dr, rows), mirrored(c, dc, cols)
        return rr * cols + cc, {"row": rr, "col": cc}

    def send_meta(peers):
        for dr, dc in peers:
            number, where = apart(dr, dc)
            pltpu.make_async_remote_copy(
                src_ref=msend.at[number], dst_ref=rm.at[dr * cols + c],
                send_sem=m_sem.at[0], recv_sem=m_sem.at[1],
                device_id=where, device_id_type=MESH,
            ).start()

    def exchange_values():
        for dr, dc in all_order:
            number, where = apart(dr, dc)
            pltpu.make_async_remote_copy(
                src_ref=vsend.at[number, pl.ds(0, cols + 1)],
                dst_ref=rv.at[dr * cols + dc, pl.ds(0, cols + 1)],
                send_sem=v_send.at[0], recv_sem=v_recv.at[dr],
                device_id=where, device_id_type=MESH,
            ).start()

    def values_of(send, recv, first, count):
        held = rv.at[pl.ds(first, count), pl.ds(0, cols + 1)]
        return pltpu.make_async_remote_copy(
            src_ref=held, dst_ref=held, send_sem=send, recv_sem=recv,
            device_id={"row": turned(r, 1, rows), "col": c}, device_id_type=MESH,
        )

    def settle(ref, first, count, sem):
        done = ref.at[pl.ds(first, count)]
        copy = pltpu.make_async_remote_copy(
            src_ref=done, dst_ref=done, send_sem=sem.at[0], recv_sem=sem.at[1],
            device_id={"row": turned(r, 1, rows), "col": c}, device_id_type=MESH,
        )
        return copy

    def side(n):
        dr, dc = SIDES[n]
        rr, cc = r + dr, c + dc
        ok = (rr >= 0) & (rr < rows) & (cc >= 0) & (cc < cols)
        return ok, {"row": jnp.clip(rr, 0, rows - 1), "col": jnp.clip(cc, 0, cols - 1)}

    def side_copy(pick, send, recv, n, incoming):
        slot = n if incoming else SIDES.index((-SIDES[n][0], -SIDES[n][1]))
        src, dst = pick(n, slot)
        return pltpu.make_async_remote_copy(
            src_ref=src, dst_ref=dst, send_sem=send.at[n], recv_sem=recv.at[slot],
            device_id=side(n)[1], device_id_type=MESH,
        )

    def sides_start(pick, send, recv):
        for n in range(len(SIDES)):
            @pl.when(side(n)[0])
            def _():
                side_copy(pick, send, recv, n, False).start()

    def sides_wait(pick, send, recv):
        for n in range(len(SIDES)):
            @pl.when(side(n)[0])
            def _():
                side_copy(pick, send, recv, n, True).wait_recv()
                side_copy(pick, send, recv, n, False).wait_send()

    def kappa_sides(n, slot):
        return kappa_ref, kb.at[slot]

    def field_sides(n, slot):
        if 0 in SIDES[n]:
            return brick, hb.at[slot]
        return corner.at[n], hc.at[slot]

    def corner_cells(dr, dc):
        far_x = [CX - x if dr > 0 else x + 1 for x in range(CX)]
        far_y = [CY - y if dc > 0 else y + 1 for y in range(CY)]
        return [(x, y) for x in range(CX) for y in range(CY) if far_x[x] + far_y[y] <= 4]

    for load in loads[:2]:
        load.wait()
    per = tile // points
    taps = TILE_ROWS * kmax
    tall = TILE_ROWS * nvec
    groups = rows // per
    stages = [range(groups // 2), range(groups // 2, groups)]

    def columns(g):
        return mirrored(r // per, g, groups)

    def limits(stage):
        lane = iota((1, len(stage) * taps), 1)
        most = jnp.zeros((1, len(stage) * taps), jnp.int32)
        for i, g in enumerate(stage):
            for a in range(TILE_ROWS):
                ours = lane // kmax == i * TILE_ROWS + a
                most = jnp.where(ours, rank_ref[a * TILE_COLS + columns(g)], most)
        return lane % kmax < most

    within = [limits(stage) for stage in stages]

    def arrive(stage):
        for g in stage:
            for k in range(g * per, (g + 1) * per):
                if k:
                    s = mirrored(r, k, rows)
                    pltpu.make_async_remote_copy(
                        src_ref=xg.at[s], dst_ref=xg.at[s], send_sem=ag_send.at[0],
                        recv_sem=ag_recv.at[k], device_id={"row": s, "col": c},
                        device_id_type=MESH,
                    ).wait_recv()

    def project(stage, kept):
        high = len(stage) * nvec
        for g in stage:
            for j in range(per):
                for q in range(subs):
                    at = j * points + q * leaf
                    x32[nvec * g : nvec * (g + 1), at : at + leaf] = xg[
                        columns(g) * per + j, q
                    ].astype(F32)
        right = jnp.concatenate(
            [right_ref[:, columns(g)].reshape(taps, tile) for g in stage], axis=0
        )
        x_rows = x32[nvec * stage[0] : nvec * (stage[-1] + 1), :].astype(BF16)
        seen = dot_nt(x_rows, right)
        row, lane = iota(seen.shape, 0), iota(seen.shape, 1)
        seen = jnp.where((row // nvec == lane // taps) & kept, seen, 0.0)
        part, lane = iota((tall, seen.shape[1]), 0), iota((tall, seen.shape[1]), 1)
        spread = jnp.zeros(part.shape, F32)
        for v in range(nvec):
            ours = jnp.sum(jnp.where(row % nvec == v, seen, 0.0), axis=0, keepdims=True)
            spread = jnp.where(part % nvec == v, ours, spread)
        spread = jnp.where(lane % taps // kmax == part // nvec, spread, 0.0)
        return spread.astype(BF16)

    def expand(stage, spread):
        left = jnp.concatenate(
            [left_ref[:, columns(g)].reshape(taps, tile) for g in stage], axis=0
        )
        return jnp.dot(spread, left, preferred_element_type=F32)

    arrive(stages[0])
    met = len(stages[0]) * per
    send_meta([d for d in all_order if d[0] < met])
    rm[c] = msend[me]
    far_rows = expand(stages[0], project(stages[0], within[0]))
    loads[2].wait()
    own_kappa.wait()
    arrive(stages[1])
    later = [d for d in all_order if d[0] >= met]
    late = project(stages[1], within[1])
    halves = 2
    side_len = leaf // halves
    straight = [jnp.zeros((row_leaves * nvec, leaf), F32) for _ in range(halves)]
    turned_near = [jnp.zeros((side_len, row_leaves * nvec), F32) for _ in range(halves)]

    def picked(l):
        column = places_ref[1, l]
        held = xg[column // subs, column % subs].astype(F32)
        spread = jnp.where(near_rows % nvec == 0, held[0:1], held[1:2])
        return jnp.where(near_rows // nvec == places_ref[0, l], spread, 0.0).astype(BF16)

    cuts = [slice(h * side_len, (h + 1) * side_len) for h in range(halves)]
    for l in range(0, nleaf, 2):
        flat, tall_x = picked(l), picked(l + 1)
        turned_near[0] += dot_nt(leaf_ref[l, cuts[0], cuts[0]], flat[:, cuts[0]])
        send_meta(later[:2])
        later = later[2:]
        turned_near[1] += dot_nt(leaf_ref[l, cuts[1], cuts[0]], flat[:, cuts[0]])
        send_meta(later[:2])
        later = later[2:]
        straight[0] += dot_nt(tall_x[:, cuts[0]], leaf_ref[l + 1, :, cuts[0]])
        send_meta(later[:2])
        later = later[2:]
        turned_near[0] += dot_nt(leaf_ref[l, cuts[0], cuts[1]], flat[:, cuts[1]])
        send_meta(later[:2])
        later = later[2:]
        turned_near[1] += dot_nt(leaf_ref[l, cuts[1], cuts[1]], flat[:, cuts[1]])
        send_meta(later[:2])
        later = later[2:]
        straight[1] += dot_nt(tall_x[:, cuts[1]], leaf_ref[l + 1, :, cuts[1]])
        send_meta(later[:2])
        later = later[2:]
        if l == nleaf // 2:
            far_rows += expand(stages[1], late)
    near = straight[0] + straight[1]
    send_meta(later)
    near += jnp.concatenate(turned_near, axis=0).T
    per_tile = tile // leaf
    packs, tops = [], []
    for j in range(cols):
        sums = []
        for q in range(subs):
            i = j * subs + q
            at = i % per_tile * leaf
            a = i // per_tile
            sums.append(
                far_rows[nvec * a : nvec * (a + 1), at : at + leaf]
                + near[nvec * i : nvec * (i + 1)]
            )
        sums = jnp.concatenate(sums, axis=1)
        tops.append(jnp.max(jnp.abs(sums), axis=0, keepdims=True))
        terms = pieces(sums)
        left_side = jnp.concatenate(
            [
                jnp.concatenate(
                    [
                        dest_hot[:, (j * blocks + b) * LANES : (j * blocks + b + 1) * LANES]
                        * jnp.broadcast_to(
                            term[v : v + 1, b * LANES : (b + 1) * LANES].astype(F32),
                            (devices, LANES),
                        ).astype(BF16)
                        for b in range(blocks)
                    ],
                    axis=1,
                )
                for term in terms
                for v in range(nvec)
            ],
            axis=0,
        )
        packed = dot_nt(left_side, slot_hot[:, j * points : (j + 1) * points])
        packs.append(packed[: nvec * devices] + packed[nvec * devices :])
    top = jnp.max(functools.reduce(jnp.maximum, tops), axis=1, keepdims=True)
    grade = jnp.ceil(jnp.log2(jnp.maximum(top, 1e-30)) * 8.0 + 0.01).astype(jnp.int32)
    grade = jnp.broadcast_to(grade, (devices, LANES))
    for j in range(cols):
        vsend[:, j, :] = coded(
            [packs[j][v * devices : (v + 1) * devices] for v in range(nvec)], grade
        )
    vsend[:, cols, :] = grade
    exchange_values()
    sides_start(kappa_sides, k_send, k_recv)
    metas = settle(rm, 1, devices - 1, m_sem)
    metas.wait_recv()
    cell_rows = iota((cells, LANES), 0).astype(F32)
    for s in range(devices):
        lane_hot[:, s * LANES : (s + 1) * LANES] = (rm[s, 1:2, :] == lane_rows).astype(BF16)
        hit_hot[:, s * LANES : (s + 1) * LANES] = (rm[s, 0:1, :] == cell_rows).astype(BF16)
    field = jnp.zeros((2 * nvec * cells, LANES), F32)
    for dr in range(rows):
        first = 0 if dr else 1
        values_of(v_send.at[0], v_recv.at[dr], dr * cols + first, cols - first).wait_recv()
        totals = [jnp.zeros((cols, LANES), F32) for _ in range(nvec)]
        for dc in range(cols):
            held = rv.at[dr * cols + dc] if dr + dc else vsend.at[me]
            parts = decoded(held[0:cols, :], held[cols : cols + 1, :])
            totals = [total + part for total, part in zip(totals, parts)]
        terms = [pieces(total) for total in totals]
        placed = [
            jnp.concatenate(
                [
                    hit_hot[:, (dr * cols + j) * LANES : (dr * cols + j + 1) * LANES]
                    * jnp.broadcast_to(
                        terms[v][i][j : j + 1, :].astype(F32), (cells, LANES)
                    ).astype(BF16)
                    for j in range(cols)
                ],
                axis=1,
            )
            for i in range(2)
            for v in range(nvec)
        ]
        span = slice(dr * cols * LANES, (dr + 1) * cols * LANES)
        field += dot_nt(jnp.concatenate(placed, axis=0), lane_hot[:, span])
    field = field[: nvec * cells] + field[nvec * cells :]
    for v in range(nvec):
        brick[v] = field[v * cells : (v + 1) * cells]
    corners = [n for n in range(len(SIDES)) if 0 not in SIDES[n]]
    for n in corners:
        held = corner_cells(*SIDES[n])
        for v in range(nvec):
            for i, (x, y) in enumerate(held):
                j, cell = v * len(held) + i, v * cells + x * CY + y
                corner[n, j // 4, j % 4 : j % 4 + 1, :] = field[cell : cell + 1]
    sides_start(field_sides, h_send, h_recv)
    rest = xg.at[pl.ds(0, rows - 1)]
    pltpu.make_async_remote_copy(
        src_ref=rest, dst_ref=rest, send_sem=ag_send.at[0], recv_sem=ag_recv.at[0],
        device_id={"row": mirrored(r, 1, rows), "col": c}, device_id_type=MESH,
    ).wait_send()
    metas.wait_send()
    values_of(v_send.at[0], v_recv.at[0], 1, devices - 1).wait_send()
    sides_wait(kappa_sides, k_send, k_recv)
    strip = 4 * CY

    def laid(ref, get, every):
        for n, (dr, dc) in enumerate(every):
            value = get(dr, dc)
            for x in range(CX):
                at_row = ((dr + 1) * CX + x) * strip + (dc + 1) * CY
                ref[at_row : at_row + CY, :] = value[x * CY : (x + 1) * CY, :]

    every = SIDES + [(0, 0)]

    def valid(dr, dc):
        return (r + dr >= 0) & (r + dr < rows) & (c + dc >= 0) & (c + dc < cols)

    def stiffness(dr, dc):
        if (dr, dc) == (0, 0):
            return (6.0 + kappa_ref[...]) * 0.125
        return jnp.where(valid(dr, dc), (6.0 + kb[SIDES.index((dr, dc))]) * 0.125, 0.0)

    laid(coef, stiffness, every)
    laid(
        scale,
        lambda dr, dc: jnp.full((cells, LANES), jnp.where(valid(dr, dc), 0.125, 0.0), F32),
        every,
    )
    sides_wait(field_sides, h_send, h_recv)

    def bricks(v, dr, dc):
        if (dr, dc) == (0, 0):
            return brick[v]
        return jnp.where(valid(dr, dc), hb[SIDES.index((dr, dc)), v], 0.0)

    for v in range(nvec):
        laid(
            ext.at[v],
            functools.partial(bricks, v),
            [near_side for near_side in every if 0 in near_side],
        )
        for n in corners:
            dr, dc = SIDES[n]
            held = corner_cells(-dr, -dc)
            for i, (x, y) in enumerate(held):
                j = v * len(held) + i
                at_row = ((dr + 1) * CX + x) * strip + (dc + 1) * CY + y
                ext[v, at_row : at_row + 1, :] = jnp.where(
                    valid(dr, dc), hc[n, j // 4, j % 4 : j % 4 + 1, :], 0.0
                )
    rows_in = ext.shape[1]
    for step in range(4):
        low = (step + 1) * strip
        count = rows_in - 2 * low
        for v in range(nvec):
            src = ext if step % 2 == 0 else work

            def at(by):
                return src[v, pl.ds(low + by, count), :]

            mid = src[v, low : low + count, :]
            z = iota(mid.shape, 1)
            beside = src[v, low + strip : low + strip + count, :]
            beside += src[v, low - strip : low - strip + count, :]
            beside += at(1) + at(-1)
            beside += jnp.where(z > 0, pltpu.roll(mid, 1, 1), 0.0)
            beside += jnp.where(z < LANES - 1, pltpu.roll(mid, LANES - 1, 1), 0.0)
            span = slice(low, low + count)
            cur = coef[span, :] * mid - scale[span, :] * beside
            if step < 3:
                (work if step % 2 == 0 else ext)[v, span, :] = cur
            else:
                out_ref[v] = cur.reshape(CX, strip, LANES)


def per_device(
    vectors, lr_left, lr_right, tile_rank, leaf_values, leaf_places, cluster_perm, kappa
):
    rows, cols = lax.axis_size("row"), lax.axis_size("col")
    devices = rows * cols
    nvec, _, points = vectors.shape
    tiles, kmax, tile = lr_left.shape[2:]
    nleaf, leaf = leaf_values.shape[2:4]
    cells, lanes = CX * CY, kappa.shape[2]
    strip, deep = 4 * CY, 3 * CX * 4 * CY
    vmem = pl.BlockSpec(memory_space=pltpu.VMEM)
    hbm = pl.BlockSpec(memory_space=pl.ANY)
    dma = pltpu.SemaphoreType.DMA
    out = pl.pallas_call(
        functools.partial(kernel, rows, cols, kmax, leaf),
        out_shape=pltpu.VMEM((nvec, CX, strip, lanes), F32),
        in_specs=[hbm] * 8,
        out_specs=vmem,
        scratch_shapes=[
            pltpu.SMEM((tiles,), jnp.int32),
            pltpu.SMEM((2, nleaf), jnp.int32),
            pltpu.VMEM((len(SIDES), 3 * nvec // 2, 4, lanes), F32),
            pltpu.VMEM((len(SIDES), 3 * nvec // 2, 4, lanes), F32),
            pltpu.VMEM((cols * points // LANES, LANES), jnp.int32),
            pltpu.VMEM((cells, lanes), F32),
            pltpu.VMEM((TILE_ROWS, TILE_COLS, kmax, tile), BF16),
            pltpu.VMEM((TILE_ROWS, TILE_COLS, kmax, tile), BF16),
            pltpu.VMEM((nleaf, leaf, leaf), BF16),
            pltpu.VMEM((rows, points // leaf, nvec, leaf), BF16),
            pltpu.VMEM((TILE_COLS * nvec, tile), F32),
            pltpu.VMEM((LANES, cols * points), BF16),
            pltpu.VMEM((devices, cols * points), BF16),
            pltpu.VMEM((devices, 2, LANES), F32),
            pltpu.VMEM((devices, 2, LANES), F32),
            pltpu.VMEM((devices, cols * nvec, LANES), jnp.int32),
            pltpu.VMEM((devices, cols * nvec, LANES), jnp.int32),
            pltpu.VMEM((LANES, devices * LANES), BF16),
            pltpu.VMEM((cells, devices * LANES), BF16),
            pltpu.VMEM((nvec, cells, lanes), F32),
            pltpu.VMEM((len(SIDES), nvec, cells, lanes), F32),
            pltpu.VMEM((len(SIDES), cells, lanes), F32),
            pltpu.VMEM((nvec, deep, lanes), F32),
            pltpu.VMEM((nvec, deep, lanes), F32),
            pltpu.VMEM((deep, lanes), F32),
            pltpu.VMEM((deep, lanes), F32),
            dma((8,)), dma((1,)), dma((rows,)), dma((2,)), dma((1,)), dma((rows,)),
            dma((len(SIDES),)), dma((len(SIDES),)), dma((len(SIDES),)), dma((len(SIDES),)),
        ],
        compiler_params=pltpu.CompilerParams(collective_id=0, has_side_effects=True),
    )(
        vectors.reshape(nvec, points // leaf, leaf).transpose(1, 0, 2),
        lr_right.reshape(TILE_ROWS, TILE_COLS, kmax, tile),
        lr_left.reshape(TILE_ROWS, TILE_COLS, kmax, tile),
        tile_rank.reshape(tiles),
        leaf_values.reshape(nleaf, leaf, leaf),
        leaf_places.reshape(nleaf, 2).T,
        cluster_perm.reshape(-1, LANES),
        kappa.reshape(cells, lanes),
    )
    return out[:, :, CY : 2 * CY, :]


def solution(mesh):
    in_specs = (
        P(None, "col", "row"),
        P("row", "col", None, None, None),
        P("row", "col", None, None, None),
        P("row", "col", None),
        P("row", "col", None, None, None),
        P("row", "col", None, None),
        P("row", None),
        P("row", "col", None),
    )
    out_specs = P(None, "row", "col", None)
    return jax.shard_map(
        per_device, mesh=mesh, in_specs=in_specs, out_specs=out_specs, check_vma=False
    )
```

```python
import functools

import jax
import jax.numpy as jnp
from jax import lax
from jax.experimental import pallas as pl
from jax.experimental.pallas import tpu as pltpu
from jax.sharding import PartitionSpec as P

CX = 4
CY = 4
TILE_ROWS = 4
TILE_COLS = 8
LANES = 128
MESH = pl.DeviceIdType.MESH
F32 = jnp.float32
BF16 = jnp.bfloat16
NT = (((1,), (1,)), ((), ()))
SIDES = [(0, -1), (0, 1), (-1, -1), (-1, 1), (1, -1), (1, 1), (-1, 0), (1, 0)]


def dot_nt(a, b):
    return lax.dot_general(a, b, NT, preferred_element_type=F32)


def pieces(x):
    first = x.astype(BF16)
    return first, (x - first.astype(F32)).astype(BF16)


def span_of(grade):
    return jnp.exp2(grade.astype(F32) * 0.125)


def coded(values, grade):
    first, second = (
        jnp.floor(v * (32000.0 / span_of(grade)) + 0.5).astype(jnp.int32) for v in values
    )
    return first * 65536 + second


def decoded(code, grade):
    second = jnp.right_shift(jnp.left_shift(code, 16), 16)
    first = jnp.right_shift(code - second, 16)
    unit = span_of(grade) * (1.0 / 32000.0)
    return first.astype(F32) * unit, second.astype(F32) * unit


def iota(shape, dim):
    return lax.broadcasted_iota(jnp.int32, shape, dim)


def kernel(
    rows, cols, kmax, leaf,
    x_hbm, right_hbm, left_hbm, rank_hbm, leaf_hbm, places_hbm, perm_hbm, kappa_hbm,
    out_ref,
    rank_ref, places_ref, corner, hc, perm_ref, kappa_ref, right_ref, left_ref, leaf_ref, xg, x32, slot_hot, dest_hot,
    msend, rm, vsend, rv, lane_hot, hit_hot, brick, hb, kb, ext, work, coef, scale,
    local_sem, ag_send, ag_recv, m_sem, v_send, v_recv, k_send, k_recv, h_send, h_recv,
):
    subs, nvec = x_hbm.shape[:2]
    points = subs * leaf
    tile = right_ref.shape[-1]
    devices = rows * cols
    nleaf = leaf_ref.shape[0]
    cells = CX * CY
    blocks = points // LANES
    r = lax.axis_index("row")
    c = lax.axis_index("col")
    me = r * cols + c

    own_x = pltpu.make_async_copy(x_hbm, xg.at[r], local_sem.at[3])
    own_perm = pltpu.make_async_copy(perm_hbm, perm_ref, local_sem.at[4])
    own_kappa = pltpu.make_async_copy(kappa_hbm, kappa_ref, local_sem.at[5])
    small = [
        pltpu.make_async_copy(rank_hbm, rank_ref, local_sem.at[6]),
        pltpu.make_async_copy(places_hbm, places_ref, local_sem.at[7]),
    ]
    loads = [
        pltpu.make_async_copy(right_hbm, right_ref, local_sem.at[0]),
        pltpu.make_async_copy(left_hbm, left_ref, local_sem.at[1]),
        pltpu.make_async_copy(leaf_hbm, leaf_ref, local_sem.at[2]),
    ]

    def turned(place, by, count):
        moved = place + by
        return moved - jnp.where(moved >= count, count, 0)

    def mirrored(place, by, count):
        if count & (count - 1):
            return turned(place, by, count)
        moved, bit = place, 1
        while bit <= by:
            if by & bit:
                moved = moved + bit - 2 * bit * (place // bit % 2)
            bit *= 2
        return moved

    def far(by):
        return bin(by).count("1")

    row_order = sorted(range(1, rows), key=lambda k: -k)
    col_order = sorted(range(1, cols), key=lambda k: -far(k))
    all_order = sorted(
        ((dr, dc) for dr in range(rows) for dc in range(cols) if dr + dc),
        key=lambda d: -(d[0] // 2 + far(d[1]) + 0.5 * (d[0] % 2)),
    )

    barrier = pltpu.get_barrier_semaphore()
    for k in row_order:
        pl.semaphore_signal(
            barrier, inc=1, device_id={"row": mirrored(r, k, rows), "col": c}, device_id_type=MESH
        )
    for k in col_order:
        pl.semaphore_signal(
            barrier, inc=1, device_id={"row": r, "col": mirrored(c, k, cols)}, device_id_type=MESH
        )
    for load in [own_x, own_perm] + small + [own_kappa] + loads:
        load.start()
    own_x.wait()
    pl.semaphore_wait(barrier, rows + cols - 2)
    for k in row_order:
        pltpu.make_async_remote_copy(
            src_ref=xg.at[r], dst_ref=xg.at[r], send_sem=ag_send.at[0], recv_sem=ag_recv.at[k],
            device_id={"row": mirrored(r, k, rows), "col": c}, device_id_type=MESH,
        ).start()

    own_perm.wait()
    dev_ids = iota((devices, LANES), 0)
    lane_rows = iota((LANES, LANES), 0).astype(F32)
    ahead = (iota((LANES, 2 * LANES), 0) < iota((LANES, 2 * LANES), 1)).astype(BF16)
    for j in range(cols):
        dev_of = perm_ref[j * blocks : (j + 1) * blocks, :] // points
        hots = [(dev_of[b : b + 1, :] == dev_ids).astype(F32) for b in range(blocks)]
        all_hot = jnp.concatenate(hots, axis=0).astype(BF16)
        counts = jnp.dot(all_hot, ahead, preferred_element_type=F32)
        offset = jnp.zeros((devices, LANES), F32)
        for b in range(blocks):
            span = slice(b * devices, (b + 1) * devices)
            at = (j * blocks + b) * LANES
            rank = jnp.sum(hots[b] * (counts[span, :LANES] + offset), axis=0, keepdims=True)
            offset = offset + counts[span, LANES:]
            slot_hot[:, at : at + LANES] = (rank == lane_rows).astype(BF16)
            dest_hot[:, at : at + LANES] = all_hot[span]
    mine = pl.ds(pl.multiple_of(c * points, LANES), points)
    place = perm_ref[pl.ds(pl.multiple_of(c * blocks, 8), blocks), :] % points
    halves = ((place // LANES).astype(F32), (place % LANES).astype(F32))
    dest_mine = dest_hot[:, mine]
    meta = jnp.concatenate(
        [
            jnp.concatenate(
                [
                    dest_mine[:, b * LANES : (b + 1) * LANES]
                    * jnp.broadcast_to(half[b : b + 1, :], (devices, LANES)).astype(BF16)
                    for b in range(blocks)
                ],
                axis=1,
            )
            for half in halves
        ],
        axis=0,
    )
    meta = dot_nt(meta, slot_hot[:, mine])
    for h in range(2):
        msend[:, h, :] = meta[h * devices : (h + 1) * devices]
    for load in small:
        load.wait()
    ext[...] = jnp.zeros_like(ext)
    coef[...] = jnp.zeros_like(coef)
    scale[...] = jnp.zeros_like(scale)
    row_leaves = cols * points // leaf
    near_rows = iota((row_leaves * nvec, leaf), 0)

    ext[...] = jnp.zeros_like(ext)
    coef[...] = jnp.zeros_like(coef)
    scale[...] = jnp.zeros_like(scale)

    def apart(dr, dc):
        rr, cc = mirrored(r, dr, rows), mirrored(c, dc, cols)
        return rr * cols + cc, {"row": rr, "col": cc}

    def send_meta(peers):
        for dr, dc in peers:
            number, where = apart(dr, dc)
            pltpu.make_async_remote_copy(
                src_ref=msend.at[number], dst_ref=rm.at[dr * cols + c],
                send_sem=m_sem.at[0], recv_sem=m_sem.at[1],
                device_id=where, device_id_type=MESH,
            ).start()

    def exchange_values():
        for dr, dc in all_order:
            number, where = apart(dr, dc)
            pltpu.make_async_remote_copy(
                src_ref=vsend.at[number, pl.ds(0, cols + 1)],
                dst_ref=rv.at[dr * cols + dc, pl.ds(0, cols + 1)],
                send_sem=v_send.at[0], recv_sem=v_recv.at[dr],
                device_id=where, device_id_type=MESH,
            ).start()

    def values_of(send, recv, first, count):
        held = rv.at[pl.ds(first, count), pl.ds(0, cols + 1)]
        return pltpu.make_async_remote_copy(
            src_ref=held, dst_ref=held, send_sem=send, recv_sem=recv,
            device_id={"row": turned(r, 1, rows), "col": c}, device_id_type=MESH,
        )

    def settle(ref, first, count, sem):
        done = ref.at[pl.ds(first, count)]
        copy = pltpu.make_async_remote_copy(
            src_ref=done, dst_ref=done, send_sem=sem.at[0], recv_sem=sem.at[1],
            device_id={"row": turned(r, 1, rows), "col": c}, device_id_type=MESH,
        )
        return copy

    def side(n):
        dr, dc = SIDES[n]
        rr, cc = r + dr, c + dc
        ok = (rr >= 0) & (rr < rows) & (cc >= 0) & (cc < cols)
        return ok, {"row": jnp.clip(rr, 0, rows - 1), "col": jnp.clip(cc, 0, cols - 1)}

    def side_copy(pick, send, recv, n, incoming):
        slot = n if incoming else SIDES.index((-SIDES[n][0], -SIDES[n][1]))
        src, dst = pick(n, slot)
        return pltpu.make_async_remote_copy(
            src_ref=src, dst_ref=dst, send_sem=send.at[n], recv_sem=recv.at[slot],
            device_id=side(n)[1], device_id_type=MESH,
        )

    def sides_start(pick, send, recv):
        for n in range(len(SIDES)):
            @pl.when(side(n)[0])
            def _():
                side_copy(pick, send, recv, n, False).start()

    def sides_wait(pick, send, recv):
        for n in range(len(SIDES)):
            @pl.when(side(n)[0])
            def _():
                side_copy(pick, send, recv, n, True).wait_recv()
                side_copy(pick, send, recv, n, False).wait_send()

    def kappa_sides(n, slot):
        return kappa_ref, kb.at[slot]

    def field_sides(n, slot):
        if 0 in SIDES[n]:
            return brick, hb.at[slot]
        return corner.at[n], hc.at[slot]

    def corner_cells(dr, dc):
        far_x = [CX - x if dr > 0 else x + 1 for x in range(CX)]
        far_y = [CY - y if dc > 0 else y + 1 for y in range(CY)]
        return [(x, y) for x in range(CX) for y in range(CY) if far_x[x] + far_y[y] <= 4]

    for load in loads[:2]:
        load.wait()
    per = tile // points
    taps = TILE_ROWS * kmax
    tall = TILE_ROWS * nvec
    groups = rows // per
    stages = [range(groups // 2), range(groups // 2, groups)]

    def columns(g):
        return mirrored(r // per, g, groups)

    def limits(stage):
        lane = iota((1, len(stage) * taps), 1)
        most = jnp.zeros((1, len(stage) * taps), jnp.int32)
        for i, g in enumerate(stage):
            for a in range(TILE_ROWS):
                ours = lane // kmax == i * TILE_ROWS + a
                most = jnp.where(ours, rank_ref[a * TILE_COLS + columns(g)], most)
        return lane % kmax < most

    within = [limits(stage) for stage in stages]

    def arrive(stage):
        for g in stage:
            for k in range(g * per, (g + 1) * per):
                if k:
                    s = mirrored(r, k, rows)
                    pltpu.make_async_remote_copy(
                        src_ref=xg.at[s], dst_ref=xg.at[s], send_sem=ag_send.at[0],
                        recv_sem=ag_recv.at[k], device_id={"row": s, "col": c},
                        device_id_type=MESH,
                    ).wait_recv()

    def project(stage, kept):
        high = len(stage) * nvec
        for g in stage:
            for j in range(per):
                for q in range(subs):
                    at = j * points + q * leaf
                    x32[nvec * g : nvec * (g + 1), at : at + leaf] = xg[
                        columns(g) * per + j, q
                    ].astype(F32)
        right = jnp.concatenate(
            [right_ref[:, columns(g)].reshape(taps, tile) for g in stage], axis=0
        )
        x_rows = x32[nvec * stage[0] : nvec * (stage[-1] + 1), :].astype(BF16)
        seen = dot_nt(x_rows, right)
        row, lane = iota(seen.shape, 0), iota(seen.shape, 1)
        seen = jnp.where((row // nvec == lane // taps) & kept, seen, 0.0)
        part, lane = iota((tall, seen.shape[1]), 0), iota((tall, seen.shape[1]), 1)
        spread = jnp.zeros(part.shape, F32)
        for v in range(nvec):
            ours = jnp.sum(jnp.where(row % nvec == v, seen, 0.0), axis=0, keepdims=True)
            spread = jnp.where(part % nvec == v, ours, spread)
        spread = jnp.where(lane % taps // kmax == part // nvec, spread, 0.0)
        return spread.astype(BF16)

    def expand(stage, spread):
        left = jnp.concatenate(
            [left_ref[:, columns(g)].reshape(taps, tile) for g in stage], axis=0
        )
        return jnp.dot(spread, left, preferred_element_type=F32)

    arrive(stages[0])
    met = len(stages[0]) * per
    send_meta([d for d in all_order if d[0] < met])
    rm[c] = msend[me]
    far_rows = expand(stages[0], project(stages[0], within[0]))
    loads[2].wait()
    own_kappa.wait()
    arrive(stages[1])
    later = [d for d in all_order if d[0] >= met]
    late = project(stages[1], within[1])
    halves = 2
    side_len = leaf // halves
    straight = [jnp.zeros((row_leaves * nvec, leaf), F32) for _ in range(halves)]
    turned_near = [jnp.zeros((side_len, row_leaves * nvec), F32) for _ in range(halves)]

    def picked(l):
        column = places_ref[1, l]
        held = xg[column // subs, column % subs].astype(F32)
        spread = jnp.where(near_rows % nvec == 0, held[0:1], held[1:2])
        return jnp.where(near_rows // nvec == places_ref[0, l], spread, 0.0).astype(BF16)

    cuts = [slice(h * side_len, (h + 1) * side_len) for h in range(halves)]
    for l in range(0, nleaf, 2):
        flat, tall_x = picked(l), picked(l + 1)
        turned_near[0] += dot_nt(leaf_ref[l, cuts[0], cuts[0]], flat[:, cuts[0]])
        send_meta(later[:2])
        later = later[2:]
        turned_near[1] += dot_nt(leaf_ref[l, cuts[1], cuts[0]], flat[:, cuts[0]])
        send_meta(later[:2])
        later = later[2:]
        straight[0] += dot_nt(tall_x[:, cuts[0]], leaf_ref[l + 1, :, cuts[0]])
        send_meta(later[:2])
        later = later[2:]
        turned_near[0] += dot_nt(leaf_ref[l, cuts[0], cuts[1]], flat[:, cuts[1]])
        send_meta(later[:2])
        later = later[2:]
        turned_near[1] += dot_nt(leaf_ref[l, cuts[1], cuts[1]], flat[:, cuts[1]])
        send_meta(later[:2])
        later = later[2:]
        straight[1] += dot_nt(tall_x[:, cuts[1]], leaf_ref[l + 1, :, cuts[1]])
        send_meta(later[:2])
        later = later[2:]
        if l == nleaf // 2:
            far_rows += expand(stages[1], late)
    near = straight[0] + straight[1]
    send_meta(later)
    near += jnp.concatenate(turned_near, axis=0).T
    per_tile = tile // leaf
    packs, tops = [], []
    for j in range(cols):
        sums = []
        for q in range(subs):
            i = j * subs + q
            at = i % per_tile * leaf
            a = i // per_tile
            sums.append(
                far_rows[nvec * a : nvec * (a + 1), at : at + leaf]
                + near[nvec * i : nvec * (i + 1)]
            )
        sums = jnp.concatenate(sums, axis=1)
        tops.append(jnp.max(jnp.abs(sums), axis=0, keepdims=True))
        terms = pieces(sums)
        left_side = jnp.concatenate(
            [
                jnp.concatenate(
                    [
                        dest_hot[:, (j * blocks + b) * LANES : (j * blocks + b + 1) * LANES]
                        * jnp.broadcast_to(
                            term[v : v + 1, b * LANES : (b + 1) * LANES].astype(F32),
                            (devices, LANES),
                        ).astype(BF16)
                        for b in range(blocks)
                    ],
                    axis=1,
                )
                for term in terms
                for v in range(nvec)
            ],
            axis=0,
        )
        packed = dot_nt(left_side, slot_hot[:, j * points : (j + 1) * points])
        packs.append(packed[: nvec * devices] + packed[nvec * devices :])
    top = jnp.max(functools.reduce(jnp.maximum, tops), axis=1, keepdims=True)
    grade = jnp.ceil(jnp.log2(jnp.maximum(top, 1e-30)) * 8.0 + 0.01).astype(jnp.int32)
    grade = jnp.broadcast_to(grade, (devices, LANES))
    for j in range(cols):
        vsend[:, j, :] = coded(
            [packs[j][v * devices : (v + 1) * devices] for v in range(nvec)], grade
        )
    vsend[:, cols, :] = grade
    exchange_values()
    sides_start(kappa_sides, k_send, k_recv)
    metas = settle(rm, 1, devices - 1, m_sem)
    metas.wait_recv()
    cell_rows = iota((cells, LANES), 0).astype(F32)
    for s in range(devices):
        lane_hot[:, s * LANES : (s + 1) * LANES] = (rm[s, 1:2, :] == lane_rows).astype(BF16)
        hit_hot[:, s * LANES : (s + 1) * LANES] = (rm[s, 0:1, :] == cell_rows).astype(BF16)
    field = jnp.zeros((2 * nvec * cells, LANES), F32)
    for dr in range(rows):
        first = 0 if dr else 1
        values_of(v_send.at[0], v_recv.at[dr], dr * cols + first, cols - first).wait_recv()
        totals = [jnp.zeros((cols, LANES), F32) for _ in range(nvec)]
        for dc in range(cols):
            held = rv.at[dr * cols + dc] if dr + dc else vsend.at[me]
            parts = decoded(held[0:cols, :], held[cols : cols + 1, :])
            totals = [total + part for total, part in zip(totals, parts)]
        terms = [pieces(total) for total in totals]
        placed = [
            jnp.concatenate(
                [
                    hit_hot[:, (dr * cols + j) * LANES : (dr * cols + j + 1) * LANES]
                    * jnp.broadcast_to(
                        terms[v][i][j : j + 1, :].astype(F32), (cells, LANES)
                    ).astype(BF16)
                    for j in range(cols)
                ],
                axis=1,
            )
            for i in range(2)
            for v in range(nvec)
        ]
        span = slice(dr * cols * LANES, (dr + 1) * cols * LANES)
        field += dot_nt(jnp.concatenate(placed, axis=0), lane_hot[:, span])
    field = field[: nvec * cells] + field[nvec * cells :]
    for v in range(nvec):
        brick[v] = field[v * cells : (v + 1) * cells]
    corners = [n for n in range(len(SIDES)) if 0 not in SIDES[n]]
    for n in corners:
        held = corner_cells(*SIDES[n])
        for v in range(nvec):
            for i, (x, y) in enumerate(held):
                j, cell = v * len(held) + i, v * cells + x * CY + y
                corner[n, j // 4, j % 4 : j % 4 + 1, :] = field[cell : cell + 1]
    sides_start(field_sides, h_send, h_recv)
    rest = xg.at[pl.ds(0, rows - 1)]
    pltpu.make_async_remote_copy(
        src_ref=rest, dst_ref=rest, send_sem=ag_send.at[0], recv_sem=ag_recv.at[0],
        device_id={"row": mirrored(r, 1, rows), "col": c}, device_id_type=MESH,
    ).wait_send()
    metas.wait_send()
    values_of(v_send.at[0], v_recv.at[0], 1, devices - 1).wait_send()
    sides_wait(kappa_sides, k_send, k_recv)
    strip = 4 * CY

    def laid(ref, get, every):
        for n, (dr, dc) in enumerate(every):
            value = get(dr, dc)
            for x in range(CX):
                at_row = ((dr + 1) * CX + x) * strip + (dc + 1) * CY
                ref[at_row : at_row + CY, :] = value[x * CY : (x + 1) * CY, :]

    every = SIDES + [(0, 0)]

    def valid(dr, dc):
        return (r + dr >= 0) & (r + dr < rows) & (c + dc >= 0) & (c + dc < cols)

    def stiffness(dr, dc):
        if (dr, dc) == (0, 0):
            return (6.0 + kappa_ref[...]) * 0.125
        return jnp.where(valid(dr, dc), (6.0 + kb[SIDES.index((dr, dc))]) * 0.125, 0.0)

    laid(coef, stiffness, every)
    laid(
        scale,
        lambda dr, dc: jnp.full((cells, LANES), jnp.where(valid(dr, dc), 0.125, 0.0), F32),
        every,
    )
    sides_wait(field_sides, h_send, h_recv)

    def bricks(v, dr, dc):
        if (dr, dc) == (0, 0):
            return brick[v]
        return jnp.where(valid(dr, dc), hb[SIDES.index((dr, dc)), v], 0.0)

    for v in range(nvec):
        laid(
            ext.at[v],
            functools.partial(bricks, v),
            [near_side for near_side in every if 0 in near_side],
        )
        for n in corners:
            dr, dc = SIDES[n]
            held = corner_cells(-dr, -dc)
            for i, (x, y) in enumerate(held):
                j = v * len(held) + i
                at_row = ((dr + 1) * CX + x) * strip + (dc + 1) * CY + y
                ext[v, at_row : at_row + 1, :] = jnp.where(
                    valid(dr, dc), hc[n, j // 4, j % 4 : j % 4 + 1, :], 0.0
                )
    rows_in = ext.shape[1]
    for step in range(4):
        low = (step + 1) * strip
        count = rows_in - 2 * low
        for v in range(nvec):
            src = ext if step % 2 == 0 else work

            def at(by):
                return src[v, pl.ds(low + by, count), :]

            mid = src[v, low : low + count, :]
            z = iota(mid.shape, 1)
            beside = src[v, low + strip : low + strip + count, :]
            beside += src[v, low - strip : low - strip + count, :]
            beside += at(1) + at(-1)
            beside += jnp.where(z > 0, pltpu.roll(mid, 1, 1), 0.0)
            beside += jnp.where(z < LANES - 1, pltpu.roll(mid, LANES - 1, 1), 0.0)
            span = slice(low, low + count)
            cur = coef[span, :] * mid - scale[span, :] * beside
            if step < 3:
                (work if step % 2 == 0 else ext)[v, span, :] = cur
            else:
                out_ref[v] = cur.reshape(CX, strip, LANES)


def per_device(
    vectors, lr_left, lr_right, tile_rank, leaf_values, leaf_places, cluster_perm, kappa
):
    rows, cols = lax.axis_size("row"), lax.axis_size("col")
    devices = rows * cols
    nvec, _, points = vectors.shape
    tiles, kmax, tile = lr_left.shape[2:]
    nleaf, leaf = leaf_values.shape[2:4]
    cells, lanes = CX * CY, kappa.shape[2]
    strip, deep = 4 * CY, 3 * CX * 4 * CY
    vmem = pl.BlockSpec(memory_space=pltpu.VMEM)
    hbm = pl.BlockSpec(memory_space=pl.ANY)
    dma = pltpu.SemaphoreType.DMA
    out = pl.pallas_call(
        functools.partial(kernel, rows, cols, kmax, leaf),
        out_shape=pltpu.VMEM((nvec, CX, strip, lanes), F32),
        in_specs=[hbm] * 8,
        out_specs=vmem,
        scratch_shapes=[
            pltpu.SMEM((tiles,), jnp.int32),
            pltpu.SMEM((2, nleaf), jnp.int32),
            pltpu.VMEM((len(SIDES), 3 * nvec // 2, 4, lanes), F32),
            pltpu.VMEM((len(SIDES), 3 * nvec // 2, 4, lanes), F32),
            pltpu.VMEM((cols * points // LANES, LANES), jnp.int32),
            pltpu.VMEM((cells, lanes), F32),
            pltpu.VMEM((TILE_ROWS, TILE_COLS, kmax, tile), BF16),
            pltpu.VMEM((TILE_ROWS, TILE_COLS, kmax, tile), BF16),
            pltpu.VMEM((nleaf, leaf, leaf), BF16),
            pltpu.VMEM((rows, points // leaf, nvec, leaf), BF16),
            pltpu.VMEM((TILE_COLS * nvec, tile), F32),
            pltpu.VMEM((LANES, cols * points), BF16),
            pltpu.VMEM((devices, cols * points), BF16),
            pltpu.VMEM((devices, 2, LANES), F32),
            pltpu.VMEM((devices, 2, LANES), F32),
            pltpu.VMEM((devices, cols * nvec, LANES), jnp.int32),
            pltpu.VMEM((devices, cols * nvec, LANES), jnp.int32),
            pltpu.VMEM((LANES, devices * LANES), BF16),
            pltpu.VMEM((cells, devices * LANES), BF16),
            pltpu.VMEM((nvec, cells, lanes), F32),
            pltpu.VMEM((len(SIDES), nvec, cells, lanes), F32),
            pltpu.VMEM((len(SIDES), cells, lanes), F32),
            pltpu.VMEM((nvec, deep, lanes), F32),
            pltpu.VMEM((nvec, deep, lanes), F32),
            pltpu.VMEM((deep, lanes), F32),
            pltpu.VMEM((deep, lanes), F32),
            dma((8,)), dma((1,)), dma((rows,)), dma((2,)), dma((1,)), dma((rows,)),
            dma((len(SIDES),)), dma((len(SIDES),)), dma((len(SIDES),)), dma((len(SIDES),)),
        ],
        compiler_params=pltpu.CompilerParams(collective_id=0, has_side_effects=True),
    )(
        vectors.reshape(nvec, points // leaf, leaf).transpose(1, 0, 2),
        lr_right.reshape(TILE_ROWS, TILE_COLS, kmax, tile),
        lr_left.reshape(TILE_ROWS, TILE_COLS, kmax, tile),
        tile_rank.reshape(tiles),
        leaf_values.reshape(nleaf, leaf, leaf),
        leaf_places.reshape(nleaf, 2).T,
        cluster_perm.reshape(-1, LANES),
        kappa.reshape(cells, lanes),
    )
    return out[:, :, CY : 2 * CY, :]


def solution(mesh):
    in_specs = (
        P(None, "col", "row"),
        P("row", "col", None, None, None),
        P("row", "col", None, None, None),
        P("row", "col", None),
        P("row", "col", None, None, None),
        P("row", "col", None, None),
        P("row", None),
        P("row", "col", None),
    )
    out_specs = P(None, "row", "col", None)
    return jax.shard_map(
        per_device, mesh=mesh, in_specs=in_specs, out_specs=out_specs, check_vma=False
    )
```
